32 devices in a mesh: fz: 8 (over y, x, core), fxy: 4 (over z).
Axes of the slice: x: 2, y: 2, z: 4, core: 2. Of those that a mesh axis runs over, the one named last changes fastest.
Arguments:
- e_field: float32 [3, 64, 64, 512], P(None, 'fz', 'fxy'), may hold values from -6 to 6
- h_field: float32 [3, 64, 64, 512], P(None, 'fz', 'fxy'), may hold values from -6 to 6
- e_decay: float32 [64, 64, 512], P('fz', 'fxy'), may hold values from 0.6 to 1
- e_gain: float32 [64, 64, 512], P('fz', 'fxy'), may hold values from 0.2 to 0.6
- port_cell: int32 [8, 256], P('fz', 'fxy'), may hold values from 0 to 65535
- port_node: int32 [8, 256], P('fz', 'fxy'), may hold values from 0 to 2047
- port_conductance: float32 [8, 256], P('fz', 'fxy'), may hold values from 0.5 to 2
- inverse: float32 [8, 2048, 2048], P('fz', 'fxy'), may hold values from -1 to 2, as said below
- line_near: int32 [8, 128], P('fz'), may hold values from 0 to 2047
- line_far: int32 [8, 128], P('fz'), may hold values from 0 to 2047
- line_delay: int32 [8, 128], P('fz'), may hold values from 1 to 6
- line_imped: float32 [8, 128], P('fz'), may hold values from 0.5 to 4
- hist_near: float32 [8, 6, 128], P('fz'), may hold values from -6 to 6
- hist_far: float32 [8, 6, 128], P('fz'), may hold values from -6 to 6
Outputs:
- e_out: float32 [3, 64, 64, 512], P(None, 'fz', 'fxy')
- h_out: float32 [3, 64, 64, 512], P(None, 'fz', 'fxy')
- node_volt: float32 [8, 2048], P('fz', 'fxy')
- line_wave: float32 [8, 2, 128], P('fz')
The draws below stay inside these ranges and needn't reach their ends.
Inputs may be any that keep to these rules, and one draw needn't show every extreme that they name: inverse[s] is symmetric for every s.
All inputs are finite; a program needn't handle non-finite values.
Results may differ from the reference program's by a relative error of at most 0.00029.
Values sent between devices are 32-bit elements; how exact they have to be, the bound alone decides.
A program may use at most 64 MiB of HBM per device.

```python
import math
import jax
import jax.numpy as jnp
from jax import lax

CZ = 8
CX = 16
NY = 512
NODES = 2048
PORTS_DEV = 64
LINES = 128
DMAX = 6
STEPS = 4
NZ = 64
NX = 64
PORTS = 256
N_FZ = 8


def draw_inverse(key, part):
    first, second = jax.random.split(jax.random.fold_in(key, 7))
    noise = jax.random.normal(first, (N_FZ, NODES, NODES), jnp.float32)
    symmetric = (noise + jnp.swapaxes(noise, 1, 2)) * (0.3 / math.sqrt(2.0 * NODES))
    diagonal = jax.random.uniform(second, (N_FZ, NODES), jnp.float32, 0.8, 1.2)
    return symmetric + diagonal[:, :, None] * jnp.eye(NODES, dtype=jnp.float32)


def with_ends(drawn, own_key, low, high):
    extent = drawn.shape
    place = [jax.random.randint(jax.random.fold_in(own_key, axis), (), 0, extent[axis]) for axis in range(len(extent))]
    drawn = drawn.at[tuple(place)].set(low)
    longest = extent.index(max(extent))
    place[longest] = (place[longest] + 1) % extent[longest]
    return drawn.at[tuple(place)].set(high)


def steps_of(key, shape, pieces, least, high):
    gain, own = 1.0, jax.random.fold_in(key, 6)
    for dim, parts in pieces:
        heights = jnp.exp(jax.random.uniform(jax.random.fold_in(own, dim), (parts,), jnp.float32, least / len(pieces), high / len(pieces)))
        gain = gain * jnp.repeat(heights, shape[dim] // parts).reshape([-1 if axis == dim else 1 for axis in range(len(shape))])
    return gain


def scatter_about(rng, dims, deviation, limit, cuts=(), held_as=jnp.bfloat16):
    array = jax.random.normal(rng, dims, jnp.float32) * deviation
    if len(cuts) > 0:
        array = steps_of(rng, dims, cuts, -0.22, 0.18) * array
    return jnp.clip(array, min=-limit, max=limit).astype(held_as)


def setup_inputs(seed: int = 0) -> dict:
    splits = jax.random.split(jax.random.key(seed), 15)
    e_field = scatter_about(splits[0], (3, NZ, NX, NY), 1.0, 6.0, ((1, 8), (2, 4)), jnp.float32)
    h_field = scatter_about(splits[1], (3, NZ, NX, NY), 1.0, 6.0, ((1, 8), (2, 4)), jnp.float32)
    e_decay = jnp.clip(0.6 + 0.39999998 * jax.random.uniform(splits[2], (NZ, NX, NY), jnp.float32) ** steps_of(splits[2], (NZ, NX, NY), ((0, 8), (1, 4)), -0.2, 0.2), 0.6, 1.0)
    e_gain = jnp.clip(0.2 + 0.400000021 * jax.random.uniform(splits[3], (NZ, NX, NY), jnp.float32) ** steps_of(splits[3], (NZ, NX, NY), ((0, 8), (1, 4)), -0.2, 0.2), 0.2, 0.6)
    port_cell = with_ends(jax.random.randint(splits[4], (N_FZ, PORTS), 0, CZ * CX * NY), jax.random.fold_in(splits[4], 1), 0, (CZ * CX * NY) - 1).astype(jnp.int32)
    port_node = with_ends(jax.random.randint(splits[5], (N_FZ, PORTS), 0, NODES), jax.random.fold_in(splits[5], 1), 0, NODES - 1).astype(jnp.int32)
    port_conductance = jnp.clip(jnp.exp(math.log(2.0) - 1.3862944 * jax.random.uniform(splits[6], (N_FZ, PORTS), jnp.float32) ** steps_of(splits[6], (N_FZ, PORTS), ((0, 8), (1, 4)), -0.2, 0.2)), 0.5, 2.0)
    inverse = draw_inverse(jax.random.fold_in(splits[14], 71), 0)
    line_near = with_ends(jax.random.randint(splits[8], (N_FZ, LINES), 0, NODES), jax.random.fold_in(splits[8], 1), 0, NODES - 1).astype(jnp.int32)
    line_far = with_ends(jax.random.randint(splits[9], (N_FZ, LINES), 0, NODES), jax.random.fold_in(splits[9], 1), 0, NODES - 1).astype(jnp.int32)
    line_delay = with_ends(jax.random.randint(splits[10], (N_FZ, LINES), 1, DMAX + 1), jax.random.fold_in(splits[10], 1), 1, DMAX).astype(jnp.int32)
    line_imped = jnp.clip(jnp.exp(math.log(4.0) - 2.0794415 * jax.random.uniform(splits[11], (N_FZ, LINES), jnp.float32) ** steps_of(splits[11], (N_FZ, LINES), ((0, 8),), -0.2, 0.2)), 0.5, 4.0)
    hist_near = scatter_about(splits[12], (N_FZ, DMAX, LINES), 1.0, 6.0, ((0, 8),), jnp.float32)
    hist_far = scatter_about(splits[13], (N_FZ, DMAX, LINES), 1.0, 6.0, ((0, 8),), jnp.float32)
    return {"e_field": e_field, "h_field": h_field, "e_decay": e_decay, "e_gain": e_gain, "port_cell": port_cell, "port_node": port_node, "port_conductance": port_conductance, "inverse": inverse, "line_near": line_near, "line_far": line_far, "line_delay": line_delay, "line_imped": line_imped, "hist_near": hist_near, "hist_far": hist_far}


def forward_z(values, upper_face):
    return jnp.concatenate([values[1:], upper_face[None]], 0) - values


def forward_x(values, side_face):
    return jnp.concatenate([values[:, 1:], side_face[:, None]], 1) - values


def forward_y(values):
    return jnp.concatenate([values[:, :, 1:], jnp.zeros_like(values[:, :, :1])], 2) - values


def backward_z(values, lower_face):
    return values - jnp.concatenate([lower_face[None], values[:-1]], 0)


def backward_x(values, side_face):
    return values - jnp.concatenate([side_face[:, None], values[:, :-1]], 1)


def backward_y(values):
    return values - jnp.concatenate([jnp.zeros_like(values[:, :, :1]), values[:, :, :-1]], 2)


def curl_electric(e_field, upper_face, side_face):
    return jnp.stack([
        forward_y(e_field[2]) - forward_z(e_field[1], upper_face[1]),
        forward_z(e_field[0], upper_face[0]) - forward_x(e_field[2], side_face[1]),
        forward_x(e_field[1], side_face[0]) - forward_y(e_field[0])])


def curl_magnetic(h_field, lower_face, side_face):
    return jnp.stack([
        backward_y(h_field[2]) - backward_z(h_field[1], lower_face[1]),
        backward_z(h_field[0], lower_face[0]) - backward_x(h_field[2], side_face[1]),
        backward_x(h_field[1], side_face[0]) - backward_y(h_field[0])])


def reference(e_field, h_field, e_decay, e_gain, port_cell, port_node, port_conductance, inverse,
              line_near, line_far, line_delay, line_imped, hist_near, hist_far):
    row_index = jnp.arange(N_FZ, dtype=jnp.int32)[:, None]
    block_index = jnp.arange(PORTS, dtype=jnp.int32)[None, :] // PORTS_DEV
    z_position = row_index * CZ + port_cell // (CX * NY)
    x_position = block_index * CX + (port_cell // NY) % CX
    y_position = port_cell % NY
    flat_index = ((z_position * NX + x_position) * NY + y_position).astype(jnp.int32)
    gain_flat = e_gain.reshape(-1)
    wave_near = hist_near[:, ::-1]
    wave_far = hist_far[:, ::-1]
    upper_zero = jnp.zeros((2, NX, NY), jnp.float32)
    side_zero = jnp.zeros((2, NZ, NY), jnp.float32)
    empty_nodes = jnp.zeros((N_FZ, NODES), jnp.float32)
    for step_index in range(STEPS):
        position = (step_index - line_delay + DMAX).astype(jnp.int32)[:, None, :]
        incoming_a = jnp.take_along_axis(wave_far, position, axis=1)[:, 0]
        incoming_b = jnp.take_along_axis(wave_near, position, axis=1)[:, 0]
        far_sources = empty_nodes.at[row_index, line_far].add(-incoming_b)
        received = jnp.concatenate([jnp.zeros((1, NODES), jnp.float32), far_sources[:-1]], 0)
        ez_ports = e_field[2].reshape(-1)[flat_index]
        sources = empty_nodes.at[row_index, port_node].add(port_conductance * ez_ports)
        sources = sources + empty_nodes.at[row_index, line_near].add(-incoming_a) + received
        volts = jnp.einsum("snm,sm->sn", inverse, sources, precision=lax.Precision.HIGHEST)
        current = port_conductance * (ez_ports - volts[row_index, port_node])
        e_field = e_decay * e_field + e_gain * curl_magnetic(h_field, upper_zero, side_zero)
        vertical = e_field[2].reshape(-1).at[flat_index].add(-gain_flat[flat_index] * current)
        e_field = e_field.at[2].set(vertical.reshape(e_field.shape[1:]))
        out_near = -2.0 * volts[row_index, line_near] / line_imped - incoming_a
        volts_above = jnp.concatenate([volts[1:], jnp.zeros((1, NODES), jnp.float32)], 0)
        out_far = -2.0 * volts_above[row_index, line_far] / line_imped - incoming_b
        h_field = h_field - 0.5 * curl_electric(e_field, upper_zero, side_zero)
        wave_near = jnp.concatenate([wave_near, out_near[:, None]], 1)
        wave_far = jnp.concatenate([wave_far, out_far[:, None]], 1)
    line_wave = jnp.stack([out_near, out_far], 1)
    return e_field, h_field, volts, line_wave
```

```python
import jax
import jax.numpy as jnp
from jax import lax
from jax.experimental import pallas as pl
from jax.experimental.pallas import tpu as pltpu
from jax.sharding import PartitionSpec as P

STEPS = 4
LANES = 128
F32 = jnp.float32
BF16 = jnp.bfloat16
I32 = jnp.int32
MESH = pl.DeviceIdType.MESH
ROWS = (((1,), (0,)), ((), ()))
COLS = (((1,), (1,)), ((), ()))


def iota(shape, dim):
    return lax.broadcasted_iota(I32, shape, dim)


def parts3(x):
    a = x.astype(BF16).astype(F32)
    r = x - a
    b = r.astype(BF16).astype(F32)
    return a, b, r - b


def dot(x, y, dims=ROWS):
    return lax.dot_general(x, y, dims, preferred_element_type=F32)


def dot3(x, onehot, dims):
    rows = x.shape[0]
    parts = list(parts3(x))
    pad = -3 * rows % 16
    if pad:
        parts.append(jnp.zeros((pad, x.shape[1]), F32))
    y = dot(jnp.concatenate(parts, 0).astype(BF16), onehot, dims)
    return y[:rows] + y[rows : 2 * rows] + y[2 * rows : 3 * rows]


def fold3(x):
    a, b, c = parts3(jnp.broadcast_to(x, (16, x.shape[1])))
    r = iota(a.shape, 0)
    x = jnp.where(r == 0, a, jnp.where(r == 1, b, jnp.where(r == 2, c, 0.0)))
    return x.astype(BF16)


def sum3(y):
    return y[0:1] + y[1:2] + y[2:3]


def column(row):
    return jnp.concatenate(
        [
            jnp.broadcast_to(row[:, t : t + LANES], (LANES, LANES)).T
            for t in range(0, row.shape[1], LANES)
        ],
        0,
    )


def kernel(
    e_in, h_in, decay_in, gain_in, port_cell_in, port_node_in, port_cond_in, inv_in,
    line_near_in, line_far_in, line_delay_in, line_imped_in, hist_near_in, hist_far_in,
    e, h, volt_out, wave_out,
    port_cell, port_node, port_cond, line_near, line_far, line_delay, line_imped,
    hist_near, hist_far,
    e_top, decay, gain, gain_top, gain_send, gain_right, inv, inv2, pick, picked, own_pick,
    same, left, mat, cell_row, cell_y, row_right, y_right, node_hi, node_lo, pads,
    info_send, info, line_send, line_info, pre_send, pre, y_send, y, below, above,
    hz, ez_up, hx_send, hx, ex_send, ex, corner_send, corner_a, corner_b, acc,
    load_sem, face_ss, face_rs, info_ss, info_rs, pre_ss, pre_rs, y_ss, y_rs,
    up_ss, up_rs, down_ss, down_rs,
):
    s, j = lax.axis_index("fz"), lax.axis_index("fxy")
    ns, nj = lax.axis_size("fz"), lax.axis_size("fxy")
    above_id, below_id = lax.rem(s + 1, ns), lax.rem(s + ns - 1, ns)
    right_id, left_id = lax.rem(j + 1, nj), lax.rem(j + nj - 1, nj)
    has_above, has_below = s < ns - 1, s > 0
    has_right, has_left = j < nj - 1, j > 0
    _, cz, cx, ny = e_in.shape
    cells = cz * cx
    block, nodes = inv_in.shape[1:]
    ports = port_cell_in.shape[1]
    lines = line_near_in.shape[1]
    depth = hist_near_in.shape[0]
    pack = LANES // ports
    tiles = nj // pack
    np_ = nj * ports
    nt = np_ + 2 * lines

    loads = [
        pltpu.make_async_copy(e_in, e, load_sem.at[0]),
        pltpu.make_async_copy(gain_in, gain, load_sem.at[1]),
        pltpu.make_async_copy(h_in, h, load_sem.at[2]),
        pltpu.make_async_copy(decay_in, decay, load_sem.at[3]),
        pltpu.make_async_copy(inv_in.at[0], inv, load_sem.at[4]),
    ]
    small = (
        (port_cell_in, port_cell), (port_node_in, port_node), (port_cond_in, port_cond),
        (line_near_in, line_near), (line_far_in, line_far), (line_delay_in, line_delay),
        (line_imped_in, line_imped), (hist_near_in, hist_near), (hist_far_in, hist_far),
    )
    small = [
        pltpu.make_async_copy(src, dst, load_sem.at[5 + k])
        for k, (src, dst) in enumerate(small)
    ]
    for copy in small + loads:
        copy.start()

    e_top[...] = jnp.zeros(e_top.shape, F32)
    below[...] = jnp.zeros(below.shape, F32)
    above[...] = jnp.zeros(above.shape, F32)
    corner_a[...] = jnp.zeros(corner_a.shape, F32)
    corner_b[...] = jnp.zeros(corner_b.shape, F32)
    line_info[...] = (iota(line_info.shape, 0) == 2).astype(F32)

    barrier = pltpu.get_barrier_semaphore()
    for other in (above_id, below_id):
        for d in range(nj):
            pl.semaphore_signal(
                barrier, inc=1, device_id={"fz": other, "fxy": lax.rem(j + d, nj)},
                device_id_type=MESH,
            )
    for d in range(1, nj):
        pl.semaphore_signal(
            barrier, inc=1, device_id={"fxy": lax.rem(j + d, nj)}, device_id_type=MESH
        )

    def remote(src, dst, ss, rs, **where):
        return pltpu.make_async_remote_copy(
            src_ref=src, dst_ref=dst, send_sem=ss, recv_sem=rs,
            device_id=where, device_id_type=MESH,
        )

    def face(kind, n, src, dst, **where):
        return remote(src, dst, face_ss.at[kind, n], face_rs.at[kind, n], **where)

    def when(cond, copies, act):
        @pl.when(cond)
        def _():
            for copy in copies:
                getattr(copy, act)()

    def up_z(n):
        return face(0, n, h.at[0:2, cz - 1], hz.at[n], fz=above_id)

    def up_x(n):
        return face(1, n, hx_send.at[n], hx.at[n], fxy=right_id)

    def down_z(n):
        return face(2, n, e.at[0:2, 0], ez_up.at[n], fz=below_id)

    def down_x(n):
        return face(3, n, ex_send.at[n], ex.at[n], fxy=left_id)

    def corner_down(n):
        return face(4, n, corner_send.at[n, 0], corner_a.at[n], fz=below_id, fxy=right_id)

    def corner_up(n):
        return face(5, n, corner_send.at[n, 1], corner_b.at[n], fz=above_id, fxy=left_id)

    line_copy = face(6, 0, line_send, line_info, fz=above_id)
    gain_z = face(6, 1, gain.at[0], gain_top, fz=below_id)
    gain_x = face(6, 2, gain_send, gain_right, fxy=left_id)

    def spread(src, dst, ss, rs):
        return [
            remote(src, dst, ss.at[d - 1], rs.at[d - 1], fxy=lax.rem(j + d, nj))
            for d in range(1, nj)
        ]

    def spread_z(src, dst, ss, rs, to):
        return [
            remote(src, dst, ss.at[d], rs.at[d], fz=to, fxy=lax.rem(j + d, nj))
            for d in range(nj)
        ]

    info_copies = spread(info_send, info.at[j], info_ss, info_rs)

    def pre_copies(n):
        return spread(pre_send.at[n], pre.at[n, j], pre_ss.at[n], pre_rs.at[n])

    def y_copies(n):
        return (
            spread(y_send.at[n], y.at[n, j], y_ss.at[n], y_rs.at[n]),
            spread_z(
                y_send.at[n, :, np_ : np_ + lines], below.at[n, j],
                up_ss.at[n], up_rs.at[n], above_id,
            ),
            spread_z(
                y_send.at[n, :, np_ + lines : nt], above.at[n, j],
                down_ss.at[n], down_rs.at[n], below_id,
            ),
        )

    def send_y(n, value):
        y_send[n] = value
        y[n, j] = value
        slab, up, down = y_copies(n)
        when(has_above, up, "start")
        when(has_below, down, "start")
        for copy in slab:
            copy.start()

    def send_h(n):
        for c in range(2):
            for z in range(cz):
                hx_send[n, c, z : z + 1, :] = h[1 + c, z, cx - 1 : cx, :]
        corner_send[n, 0] = h[2, 0, cx - 1 : cx, :]
        corner_send[n, 1] = h[0, cz - 1, 0:1, :]
        when(has_above, [up_z(n)], "start")
        when(has_right, [up_x(n)], "start")
        when(has_below & has_right, [corner_down(n)], "start")
        when(has_above & has_left, [corner_up(n)], "start")

    def send_e(n):
        for c in range(2):
            for z in range(cz):
                ex_send[n, c, z : z + 1, :] = e[1 + c, z, 0:1, :]
        when(has_below, [down_z(n)], "start")
        when(has_left, [down_x(n)], "start")

    lane = iota((cx, ny), 1)
    sub = iota((cx, ny), 0)

    def update_e():
        def plane(z, lower):
            hx_, hy_, hz_ = (h[c, z] for c in range(3))
            dx, dy = hx_, hy_
            if lower is not None:
                dx, dy = hx_ - h[0, lower], hy_ - h[1, lower]

            def by(f):
                return f - jnp.where(lane == 0, 0.0, pltpu.roll(f, 1, 1))

            def bx(f):
                return f - jnp.where(sub == 0, 0.0, pltpu.roll(f, 1, 0))

            g, q = gain[z], decay[z]
            e[0, z] = q * e[0, z] + g * (by(hz_) - dy)
            e[1, z] = q * e[1, z] + g * (dx - bx(hz_))
            e[2, z] = q * e[2, z] + g * (bx(hy_) - by(hx_))

        plane(0, None)

        @pl.loop(1, cz)
        def _(z):
            plane(z, z - 1)

    def update_h():
        def plane(z, ux, uy):
            ex_, ey_, ez_ = (e[c, z] for c in range(3))

            def dy(f):
                return jnp.where(lane == ny - 1, 0.0, pltpu.roll(f, ny - 1, 1)) - f

            def dx(f):
                return jnp.where(sub == cx - 1, 0.0, pltpu.roll(f, cx - 1, 0)) - f

            h[0, z] = h[0, z] - 0.5 * (dy(ez_) - (uy - ey_))
            h[1, z] = h[1, z] - 0.5 * ((ux - ex_) - dx(ez_))
            h[2, z] = h[2, z] - 0.5 * (dx(ey_) - dy(ex_))

        @pl.loop(0, cz - 1)
        def _(z):
            plane(z, e[0, z + 1], e[1, z + 1])

        plane(cz - 1, e_top[0], e_top[1])

    for copy in small:
        copy.wait()

    pads[...] = jnp.zeros(pads.shape, F32)
    pads[0:1, 0:ports] = (port_cell[...] + 1).astype(F32)
    pads[1:2, 0:ports] = (port_node[...] + 1).astype(F32)
    pads[2:3, 0:ports] = port_cond[...]
    rows = pltpu.roll(pads[...], ports * lax.rem(j, pack), 1)
    info_send[...] = rows
    cell = rows[0:1].astype(I32) - 1
    valid = cell >= 0
    cell_row[...] = (
        iota((cells, LANES), 0) == jnp.where(valid, cell // ny, -1)
    ).astype(F32)
    cell_y[...] = (
        (iota((ny, LANES), 0) == jnp.where(valid, cell % ny, -1)).astype(F32).astype(BF16)
    )
    line_send[...] = jnp.zeros(line_send.shape, F32)
    line_send[0:1, :] = (line_far[...] + 1).astype(F32)
    line_send[1:2, :] = line_delay[...].astype(F32)
    line_send[2:3, :] = line_imped[...]
    for k in range(depth):
        line_send[3 + k : 4 + k, :] = hist_near[k]
        line_send[3 + depth + k : 4 + depth + k, :] = hist_far[k]

    def gather_cells(f):
        value = dot3(f.reshape(cells, ny), cell_y[...], ROWS)
        return jnp.sum(value * cell_row[...], axis=0, keepdims=True)

    loads[0].wait()
    info_send[4:5, :] = gather_cells(e[2])
    loads[1].wait()
    info_send[3:4, :] = gather_cells(gain[...])
    for z in range(cz):
        gain_send[z : z + 1, :] = gain[z, 0:1, :]
    info[j] = info_send[...]

    pl.semaphore_wait(barrier, nj - 1 + 2 * nj)
    for copy in info_copies:
        copy.start()
    when(has_above, [line_copy], "start")
    loads[2].wait()
    send_h(0)
    loads[3].wait()
    update_e()
    send_e(0)
    when(has_below, [gain_z], "start")
    when(has_left, [gain_x], "start")
    loads[4].wait()

    chunk = 32

    @pl.loop(0, block // chunk)
    def _(r):
        at = pl.ds(pl.multiple_of(r * chunk, chunk), chunk)
        x = inv[at, :]
        high = x.astype(BF16)
        inv2[at, :] = high
        inv2[pl.ds(pl.multiple_of(block + r * chunk, chunk), chunk), :] = (
            x - high.astype(F32)
        ).astype(BF16)

    when(has_below, [line_copy], "wait_recv")
    for copy in info_copies:
        copy.wait_recv()

    everyone = jnp.concatenate(
        [sum(info[t * pack + k] for k in range(pack)) for t in range(tiles)], 1
    )
    cell_all = everyone[0:1] - 1.0
    cond_all, gain_all = everyone[2:3], everyone[3:4]
    near_far = [line_near[...], line_info[0:1, :].astype(I32) - 1]
    index = jnp.concatenate([everyone[1:2].astype(I32) - 1, *near_far], 1)
    high = jnp.where(index >= 0, index // block, -1)
    low = jnp.where(index >= 0, index % block, -1)
    node_hi[...] = (iota(node_hi.shape, 0) == high).astype(F32)
    node_lo[...] = (iota(node_lo.shape, 0) == low).astype(F32).astype(BF16)

    delay = jnp.concatenate([line_delay[...].astype(F32), line_info[1:2, :]], 0)
    scale = -2.0 / jnp.concatenate([line_imped[...], line_info[2:3, :]], 0)
    past_a = [
        jnp.concatenate([hist_near[k], line_info[3 + k : 4 + k, :]], 0)
        for k in range(depth)
    ]
    past_b = [
        jnp.concatenate([hist_far[k], line_info[3 + depth + k : 4 + depth + k, :]], 0)
        for k in range(depth)
    ]
    waves_a, waves_b = [], []

    def incoming(n, waves, past):
        total = jnp.zeros((2, lines), F32)
        for k in range(1, depth + 1):
            value = waves[n - k] if n >= k else past[k - n - 1]
            total = jnp.where(delay == k, value, total)
        return total

    def sources(n, ez):
        in_a, in_b = incoming(n, waves_b, past_b), incoming(n, waves_a, past_a)
        return in_a, in_b, jnp.concatenate([cond_all * ez, -in_a[0:1], -in_b[1:2]], 1)

    def own_volts(src):
        totals = dot3(node_hi[...] * src, node_lo[...], COLS)[0:nj]

        @pl.loop(0, block // chunk)
        def _(r):
            at = pl.ds(pl.multiple_of(r * chunk, chunk), chunk)
            value = jnp.zeros((chunk, LANES), F32)
            for k in range(nodes // LANES):
                q, w = divmod(k * LANES, block)
                value = value + inv[at, k * LANES : (k + 1) * LANES] * totals[
                    q : q + 1, w : w + LANES
                ]
            acc[at, :] = value

        terms = jnp.concatenate(parts3(acc[...]), 1).astype(BF16)
        return dot(jnp.ones((16, 3 * LANES), BF16), terms, COLS)[0:1]

    key = cell_all + ((iota((1, np_), 1) // ports) * (cells * ny)).astype(F32)
    key_col = column(key)
    for t in range(0, np_, LANES):
        at = slice(t, t + LANES)
        same[:, at] = (key_col == key[:, at]).astype(F32) * cond_all[:, at]

    ez = everyone[4:5]
    in_a, in_b, src = sources(0, ez)
    v0 = sum3(dot(fold3(own_volts(src)), node_lo[...]))
    v0 = jnp.where(high == j, v0, 0.0)
    drive = lax.dot_general(
        jnp.broadcast_to(v0[:, 0:np_], (8, np_)), same[...], COLS,
        precision=lax.Precision.HIGHEST, preferred_element_type=F32,
    )[0:1]
    send_y(0, jnp.concatenate([gain_all * drive, v0[:, np_:]], 1))

    neighbour = info[right_id]
    cell_r = neighbour[0:1].astype(I32) - 1
    gain_r = neighbour[3:4]
    valid_r = (cell_r >= 0) & (lax.rem(cell_r // ny, cx) == 0) & has_right
    row_right[...] = (
        iota((cz, LANES), 0) == jnp.where(valid_r, cell_r // (cx * ny), -1)
    ).astype(F32)
    y_right[...] = (
        (iota((ny, LANES), 0) == jnp.where(valid_r, cell_r % ny, -1))
        .astype(F32)
        .astype(BF16)
    )

    def send_pre(n):
        value = gather_cells(e[2])
        side = dot3(hx_send[n - 1, 0], y_right[...], ROWS) * row_right[...]
        side = -gain_r * jnp.sum(side, axis=0, keepdims=True)
        for t in range(tiles):
            at = slice(t * LANES, (t + 1) * LANES)
            both = jnp.where(j // pack == t, value, 0.0)
            both = both + jnp.where(right_id // pack == t, side, 0.0)
            pre_send[n, :, at] = both
        pre[n, j] = pre_send[n]
        for copy in pre_copies(n):
            copy.start()

    send_pre(1)

    cond_col = column(cond_all)
    gain_col = column(gain_all)
    load, first = [], []
    for t in range(0, np_, LANES):
        hit = key_col == key[:, t : t + LANES]
        load.append(jnp.sum(jnp.where(hit, cond_col, 0.0), axis=0, keepdims=True))
        earlier = hit & (iota(hit.shape, 0) < iota(hit.shape, 1) + t)
        first.append(jnp.max(earlier.astype(F32), axis=0, keepdims=True))
    load = gain_all * jnp.concatenate(load, 1)
    first = 1.0 - jnp.concatenate(first, 1)

    @pl.loop(0, nodes // LANES)
    def _(r):
        at = pl.ds(pl.multiple_of(r * LANES, LANES), LANES)
        pick[at, :] = (iota((LANES, nt), 0) + r * LANES == index).astype(F32).astype(BF16)

    wide = 2 * LANES

    @pl.loop(0, nt // wide)
    def _(c):
        at = pl.ds(pl.multiple_of(c * wide, wide), wide)
        for half in range(2):
            rows = slice(half * block, (half + 1) * block)
            picked[rows, at] = dot(inv2[rows, :], pick[:, at]).astype(BF16)

    index_col = column(index.astype(F32))
    for w in range(0, block, LANES):
        node = (iota((nt, LANES), 1) + (w + j * block)).astype(F32)
        own_pick[:, w : w + LANES] = (index_col == node).astype(F32).astype(BF16)
    mixed = dot3(same[...], own_pick[0:np_, :], ROWS)
    for w in range(0, block, LANES):
        at = slice(w, w + LANES)
        value = mixed[:, at] * gain_col
        high_ = value.astype(BF16)
        left[0:np_, at] = high_
        left[np_ : 2 * np_, at] = (value - high_.astype(F32)).astype(BF16)
    left[2 * np_ :, :] = own_pick[np_:, :]
    upper = dot(left[...], picked[0:block, :])
    lower = dot(left[0:np_, :], picked[block:, :])
    value = upper[0:np_] + (upper[np_ : 2 * np_] + lower)
    high_ = value.astype(BF16)
    mat[0:np_, 0:nt] = high_
    mat[0:np_, nt:] = (value - high_.astype(F32)).astype(BF16)
    mat[np_:, 0:nt] = upper[2 * np_ :].astype(BF16)
    mat[np_:, nt:] = dot(left[2 * np_ :, :], picked[block:, :]).astype(BF16)

    def tile_of(x, device):
        out = x[:, 0:LANES]
        for t in range(1, tiles):
            out = jnp.where(device // pack == t, x[:, t * LANES : (t + 1) * LANES], out)
        return out

    when(has_above, [gain_z], "wait_recv")
    when(has_right, [gain_x], "wait_recv")
    at_x = slice(cx - 1, cx)

    for n in range(STEPS):
        slab, up, down = y_copies(n)
        for copy in slab:
            copy.wait_recv()
        when(has_below, up, "wait_recv")
        when(has_above, down, "wait_recv")
        total, v_below, v_above = y[n, 0], below[n, 0], above[n, 0]
        for k in range(1, nj):
            total = total + y[n, k]
            v_below = v_below + below[n, k]
            v_above = v_above + above[n, k]
        v_near = jnp.concatenate([total[:, np_ : np_ + lines], v_below], 0)
        v_far = jnp.concatenate([v_above, total[:, np_ + lines :]], 0)
        waves_a.append(scale * v_near - in_a)
        waves_b.append(scale * v_far - in_b)
        change = total[:, 0:np_] - load * ez
        if n + 1 < STEPS:
            for copy in pre_copies(n + 1):
                copy.wait_recv()
            ez = change + pre[n + 1, 0]
            for k in range(1, nj):
                ez = ez + pre[n + 1, k]
            in_a, in_b, src = sources(n + 1, ez)
            x = fold3(src)
            send_y(n + 1, sum3(dot(jnp.concatenate([x, x], 1), mat[...], COLS)))
        change = change * first
        drop = dot3(cell_row[...] * tile_of(change, j), cell_y[...], COLS)

        when(has_below, [down_z(n)], "wait_send")

        @pl.when(has_left)
        def _():
            up_x(n).wait_recv()
            for z in range(cz):
                g = gain[z, 0:1, :]
                e[1, z, 0:1, :] = e[1, z, 0:1, :] + g * hx[n, 1, z : z + 1, :]
                e[2, z, 0:1, :] = e[2, z, 0:1, :] - g * hx[n, 0, z : z + 1, :]

        @pl.when(has_below)
        def _():
            up_z(n).wait_recv()
            g = gain[0]
            e[0, 0] = e[0, 0] + g * hz[n, 1]
            e[1, 0] = e[1, 0] - g * hz[n, 0]

        e[2] = e[2] + drop.reshape(cz, cx, ny)
        when(has_above & has_left, [corner_down(n)], "wait_recv")
        when(has_below & has_right, [corner_up(n)], "wait_recv")

        @pl.when(has_above)
        def _():
            down_z(n).wait_recv()
            e_top[0] = ez_up[n, 0] + gain_top[...] * h[1, cz - 1]
            e_top[1] = ez_up[n, 1] - gain_top[...] * h[0, cz - 1]
            e_top[1, 0:1, :] = e_top[1, 0:1, :] + gain_top[0:1, :] * corner_a[n]
            up_z(n).wait_send()

        drop_right = dot3(row_right[...] * tile_of(change, right_id), y_right[...], COLS)
        update_h()

        @pl.when(has_right)
        def _():
            down_x(n).wait_recv()
            g = gain_right[...]
            face_y = ex[n, 0] + g * hx_send[n, 1]
            face_z = ex[n, 1] - g * hx_send[n, 0] + drop_right
            for z in range(cz):
                y_ = face_y[z : z + 1]
                if z == 0:
                    y_ = y_ - g[0:1] * corner_b[n]
                h[1, z, at_x, :] = h[1, z, at_x, :] + 0.5 * face_z[z : z + 1]
                h[2, z, at_x, :] = h[2, z, at_x, :] - 0.5 * y_

        if n + 1 < STEPS:
            send_h(n + 1)
            update_e()
            if n + 2 < STEPS:
                send_pre(n + 2)
            send_e(n + 1)
        if n + 2 == STEPS:
            volt_out[...] = own_volts(src)

    wave_out[0, 0:1, :] = waves_a[-1][0:1]
    wave_out[0, 1:2, :] = waves_b[-1][0:1]

    for copy in info_copies:
        copy.wait_send()
    when(has_above, [line_copy], "wait_send")
    when(has_below, [gain_z], "wait_send")
    when(has_left, [gain_x], "wait_send")
    for n in range(STEPS):
        slab, up, down = y_copies(n)
        for copy in slab:
            copy.wait_send()
        when(has_above, up, "wait_send")
        when(has_below, down, "wait_send")
        if n:
            for copy in pre_copies(n):
                copy.wait_send()
        when(has_right, [up_x(n)], "wait_send")
        when(has_left, [down_x(n)], "wait_send")
        when(has_below & has_right, [corner_down(n)], "wait_send")
        when(has_above & has_left, [corner_up(n)], "wait_send")


def local(*args):
    e_field, inverse = args[0], args[7]
    nj = lax.axis_size("fxy")
    _, cz, cx, ny = e_field.shape
    _, block, nodes = inverse.shape
    ports, lines = args[4].shape[1], args[8].shape[1]
    args = [*args[:12], *(a.transpose(1, 0, 2) for a in args[12:])]
    depth = args[12].shape[0]
    vmem = pl.BlockSpec(memory_space=pltpu.VMEM)
    hbm = pl.BlockSpec(memory_space=pltpu.HBM)
    small = [a for i, a in enumerate(args) if i not in (0, 1, 2, 3, 7)]
    rows = -(-nj // 16) * 16
    np_ = nj * ports
    nt = np_ + 2 * lines
    line_rows = -(-(3 + 2 * depth) // 8) * 8
    dma = pltpu.SemaphoreType.DMA
    v = pltpu.VMEM
    return pl.pallas_call(
        kernel,
        out_shape=(
            v(e_field.shape, F32),
            v(e_field.shape, F32),
            v((1, block), F32),
            v((1, 2, lines), F32),
        ),
        in_specs=[hbm] * len(args),
        out_specs=(vmem,) * 4,
        scratch_shapes=[
            *[v(a.shape, a.dtype) for a in small],
            v((2, cx, ny), F32),
            v((cz, cx, ny), F32),
            v((cz, cx, ny), F32),
            v((cx, ny), F32),
            v((cz, ny), F32),
            v((cz, ny), F32),
            v((block, nodes), F32),
            v((2 * block, nodes), BF16),
            v((nodes, nt), BF16),
            v((2 * block, nt), BF16),
            v((nt, block), BF16),
            v((np_, np_), F32),
            v((2 * np_ + 2 * lines, block), BF16),
            v((nt, 2 * nt), BF16),
            v((cz * cx, LANES), F32),
            v((ny, LANES), BF16),
            v((cz, LANES), F32),
            v((ny, LANES), BF16),
            v((rows, nt), F32),
            v((block, nt), BF16),
            v((8, LANES), F32),
            v((8, LANES), F32),
            v((nj, 8, LANES), F32),
            v((line_rows, lines), F32),
            v((line_rows, lines), F32),
            v((STEPS, 1, np_), F32),
            v((STEPS, nj, 1, np_), F32),
            v((STEPS, 1, nt), F32),
            v((STEPS, nj, 1, nt), F32),
            v((STEPS, nj, 1, lines), F32),
            v((STEPS, nj, 1, lines), F32),
            v((STEPS, 2, cx, ny), F32),
            v((STEPS, 2, cx, ny), F32),
            v((STEPS, 2, cz, ny), F32),
            v((STEPS, 2, cz, ny), F32),
            v((STEPS, 2, cz, ny), F32),
            v((STEPS, 2, cz, ny), F32),
            v((STEPS, 2, 1, ny), F32),
            v((STEPS, 1, ny), F32),
            v((STEPS, 1, ny), F32),
            v((block, LANES), F32),
            dma((5 + len(small),)),
            dma((7, STEPS)),
            dma((7, STEPS)),
            dma((nj - 1,)),
            dma((nj - 1,)),
            dma((STEPS, nj - 1)),
            dma((STEPS, nj - 1)),
            dma((STEPS, nj - 1)),
            dma((STEPS, nj - 1)),
            dma((STEPS, nj)),
            dma((STEPS, nj)),
            dma((STEPS, nj)),
            dma((STEPS, nj)),
        ],
        compiler_params=pltpu.CompilerParams(
            collective_id=0, has_side_effects=True, vmem_limit_bytes=61 * 1024 * 1024
        ),
    )(*args)


def solution(mesh):
    placed = (
        P(None, "fz", "fxy", None),
        P(None, "fz", "fxy", None),
        P("fz", "fxy", None),
        P("fz", "fxy", None),
        P("fz", "fxy"),
        P("fz", "fxy"),
        P("fz", "fxy"),
        P("fz", "fxy", None),
        P("fz", None),
        P("fz", None),
        P("fz", None),
        P("fz", None),
        P("fz", None, None),
        P("fz", None, None),
    )
    return jax.shard_map(
        local,
        mesh=mesh,
        in_specs=placed,
        out_specs=(
            P(None, "fz", "fxy", None),
            P(None, "fz", "fxy", None),
            P("fz", "fxy"),
            P("fz", None, None),
        ),
        check_vma=False,
    )
```

```python
import jax
import jax.numpy as jnp
from jax import lax
from jax.experimental import pallas as pl
from jax.experimental.pallas import tpu as pltpu
from jax.sharding import PartitionSpec as P

STEPS = 4
LANES = 128
F32 = jnp.float32
BF16 = jnp.bfloat16
I32 = jnp.int32
MESH = pl.DeviceIdType.MESH
ROWS = (((1,), (0,)), ((), ()))
COLS = (((1,), (1,)), ((), ()))


def iota(shape, dim):
    return lax.broadcasted_iota(I32, shape, dim)


def parts3(x):
    a = x.astype(BF16).astype(F32)
    r = x - a
    b = r.astype(BF16).astype(F32)
    return a, b, r - b


def dot(x, y, dims=ROWS):
    return lax.dot_general(x, y, dims, preferred_element_type=F32)


def dot3(x, onehot, dims):
    rows = x.shape[0]
    parts = list(parts3(x))
    pad = -3 * rows % 16
    if pad:
        parts.append(jnp.zeros((pad, x.shape[1]), F32))
    y = dot(jnp.concatenate(parts, 0).astype(BF16), onehot, dims)
    return y[:rows] + y[rows : 2 * rows] + y[2 * rows : 3 * rows]


def fold3(x):
    a, b, c = parts3(jnp.broadcast_to(x, (16, x.shape[1])))
    r = iota(a.shape, 0)
    x = jnp.where(r == 0, a, jnp.where(r == 1, b, jnp.where(r == 2, c, 0.0)))
    return x.astype(BF16)


def sum3(y):
    return y[0:1] + y[1:2] + y[2:3]


def column(row):
    return jnp.concatenate(
        [
            jnp.broadcast_to(row[:, t : t + LANES], (LANES, LANES)).T
            for t in range(0, row.shape[1], LANES)
        ],
        0,
    )


def kernel(
    e_in, h_in, decay_in, gain_in, port_cell_in, port_node_in, port_cond_in, inv_in,
    line_near_in, line_far_in, line_delay_in, line_imped_in, hist_near_in, hist_far_in,
    e, h, volt_out, wave_out,
    port_cell, port_node, port_cond, line_near, line_far, line_delay, line_imped,
    hist_near, hist_far,
    e_top, decay, gain, gain_top, gain_send, gain_right, inv, inv2, pick, picked, own_pick,
    same, left, mat, cell_row, cell_y, row_right, y_right, node_hi, node_lo, pads,
    info_send, info, line_send, line_info, pre_send, pre, y_send, y, below, above,
    hz, ez_up, hx_send, hx, ex_send, ex, corner_send, corner_a, corner_b, acc,
    load_sem, face_ss, face_rs, info_ss, info_rs, pre_ss, pre_rs, y_ss, y_rs,
    up_ss, up_rs, down_ss, down_rs,
):
    s, j = lax.axis_index("fz"), lax.axis_index("fxy")
    ns, nj = lax.axis_size("fz"), lax.axis_size("fxy")
    above_id, below_id = lax.rem(s + 1, ns), lax.rem(s + ns - 1, ns)
    right_id, left_id = lax.rem(j + 1, nj), lax.rem(j + nj - 1, nj)
    has_above, has_below = s < ns - 1, s > 0
    has_right, has_left = j < nj - 1, j > 0
    _, cz, cx, ny = e_in.shape
    cells = cz * cx
    block, nodes = inv_in.shape[1:]
    ports = port_cell_in.shape[1]
    lines = line_near_in.shape[1]
    depth = hist_near_in.shape[0]
    pack = LANES // ports
    tiles = nj // pack
    np_ = nj * ports
    nt = np_ + 2 * lines

    loads = [
        pltpu.make_async_copy(e_in, e, load_sem.at[0]),
        pltpu.make_async_copy(gain_in, gain, load_sem.at[1]),
        pltpu.make_async_copy(h_in, h, load_sem.at[2]),
        pltpu.make_async_copy(decay_in, decay, load_sem.at[3]),
        pltpu.make_async_copy(inv_in.at[0], inv, load_sem.at[4]),
    ]
    small = (
        (port_cell_in, port_cell), (port_node_in, port_node), (port_cond_in, port_cond),
        (line_near_in, line_near), (line_far_in, line_far), (line_delay_in, line_delay),
        (line_imped_in, line_imped), (hist_near_in, hist_near), (hist_far_in, hist_far),
    )
    small = [
        pltpu.make_async_copy(src, dst, load_sem.at[5 + k])
        for k, (src, dst) in enumerate(small)
    ]
    for copy in small + loads:
        copy.start()

    e_top[...] = jnp.zeros(e_top.shape, F32)
    below[...] = jnp.zeros(below.shape, F32)
    above[...] = jnp.zeros(above.shape, F32)
    corner_a[...] = jnp.zeros(corner_a.shape, F32)
    corner_b[...] = jnp.zeros(corner_b.shape, F32)
    line_info[...] = (iota(line_info.shape, 0) == 2).astype(F32)

    barrier = pltpu.get_barrier_semaphore()
    for other in (above_id, below_id):
        for d in range(nj):
            pl.semaphore_signal(
                barrier, inc=1, device_id={"fz": other, "fxy": lax.rem(j + d, nj)},
                device_id_type=MESH,
            )
    for d in range(1, nj):
        pl.semaphore_signal(
            barrier, inc=1, device_id={"fxy": lax.rem(j + d, nj)}, device_id_type=MESH
        )

    def remote(src, dst, ss, rs, **where):
        return pltpu.make_async_remote_copy(
            src_ref=src, dst_ref=dst, send_sem=ss, recv_sem=rs,
            device_id=where, device_id_type=MESH,
        )

    def face(kind, n, src, dst, **where):
        return remote(src, dst, face_ss.at[kind, n], face_rs.at[kind, n], **where)

    def when(cond, copies, act):
        @pl.when(cond)
        def _():
            for copy in copies:
                getattr(copy, act)()

    def up_z(n):
        return face(0, n, h.at[0:2, cz - 1], hz.at[n], fz=above_id)

    def up_x(n):
        return face(1, n, hx_send.at[n], hx.at[n], fxy=right_id)

    def down_z(n):
        return face(2, n, e.at[0:2, 0], ez_up.at[n], fz=below_id)

    def down_x(n):
        return face(3, n, ex_send.at[n], ex.at[n], fxy=left_id)

    def corner_down(n):
        return face(4, n, corner_send.at[n, 0], corner_a.at[n], fz=below_id, fxy=right_id)

    def corner_up(n):
        return face(5, n, corner_send.at[n, 1], corner_b.at[n], fz=above_id, fxy=left_id)

    line_copy = face(6, 0, line_send, line_info, fz=above_id)
    gain_z = face(6, 1, gain.at[0], gain_top, fz=below_id)
    gain_x = face(6, 2, gain_send, gain_right, fxy=left_id)

    def spread(src, dst, ss, rs):
        return [
            remote(src, dst, ss.at[d - 1], rs.at[d - 1], fxy=lax.rem(j + d, nj))
            for d in range(1, nj)
        ]

    def spread_z(src, dst, ss, rs, to):
        return [
            remote(src, dst, ss.at[d], rs.at[d], fz=to, fxy=lax.rem(j + d, nj))
            for d in range(nj)
        ]

    info_copies = spread(info_send, info.at[j], info_ss, info_rs)

    def pre_copies(n):
        return spread(pre_send.at[n], pre.at[n, j], pre_ss.at[n], pre_rs.at[n])

    def y_copies(n):
        return (
            spread(y_send.at[n], y.at[n, j], y_ss.at[n], y_rs.at[n]),
            spread_z(
                y_send.at[n, :, np_ : np_ + lines], below.at[n, j],
                up_ss.at[n], up_rs.at[n], above_id,
            ),
            spread_z(
                y_send.at[n, :, np_ + lines : nt], above.at[n, j],
                down_ss.at[n], down_rs.at[n], below_id,
            ),
        )

    def send_y(n, value):
        y_send[n] = value
        y[n, j] = value
        slab, up, down = y_copies(n)
        when(has_above, up, "start")
        when(has_below, down, "start")
        for copy in slab:
            copy.start()

    def send_h(n):
        for c in range(2):
            for z in range(cz):
                hx_send[n, c, z : z + 1, :] = h[1 + c, z, cx - 1 : cx, :]
        corner_send[n, 0] = h[2, 0, cx - 1 : cx, :]
        corner_send[n, 1] = h[0, cz - 1, 0:1, :]
        when(has_above, [up_z(n)], "start")
        when(has_right, [up_x(n)], "start")
        when(has_below & has_right, [corner_down(n)], "start")
        when(has_above & has_left, [corner_up(n)], "start")

    def send_e(n):
        for c in range(2):
            for z in range(cz):
                ex_send[n, c, z : z + 1, :] = e[1 + c, z, 0:1, :]
        when(has_below, [down_z(n)], "start")
        when(has_left, [down_x(n)], "start")

    lane = iota((cx, ny), 1)
    sub = iota((cx, ny), 0)

    def update_e():
        def plane(z, lower):
            hx_, hy_, hz_ = (h[c, z] for c in range(3))
            dx, dy = hx_, hy_
            if lower is not None:
                dx, dy = hx_ - h[0, lower], hy_ - h[1, lower]

            def by(f):
                return f - jnp.where(lane == 0, 0.0, pltpu.roll(f, 1, 1))

            def bx(f):
                return f - jnp.where(sub == 0, 0.0, pltpu.roll(f, 1, 0))

            g, q = gain[z], decay[z]
            e[0, z] = q * e[0, z] + g * (by(hz_) - dy)
            e[1, z] = q * e[1, z] + g * (dx - bx(hz_))
            e[2, z] = q * e[2, z] + g * (bx(hy_) - by(hx_))

        plane(0, None)

        @pl.loop(1, cz)
        def _(z):
            plane(z, z - 1)

    def update_h():
        def plane(z, ux, uy):
            ex_, ey_, ez_ = (e[c, z] for c in range(3))

            def dy(f):
                return jnp.where(lane == ny - 1, 0.0, pltpu.roll(f, ny - 1, 1)) - f

            def dx(f):
                return jnp.where(sub == cx - 1, 0.0, pltpu.roll(f, cx - 1, 0)) - f

            h[0, z] = h[0, z] - 0.5 * (dy(ez_) - (uy - ey_))
            h[1, z] = h[1, z] - 0.5 * ((ux - ex_) - dx(ez_))
            h[2, z] = h[2, z] - 0.5 * (dx(ey_) - dy(ex_))

        @pl.loop(0, cz - 1)
        def _(z):
            plane(z, e[0, z + 1], e[1, z + 1])

        plane(cz - 1, e_top[0], e_top[1])

    for copy in small:
        copy.wait()

    pads[...] = jnp.zeros(pads.shape, F32)
    pads[0:1, 0:ports] = (port_cell[...] + 1).astype(F32)
    pads[1:2, 0:ports] = (port_node[...] + 1).astype(F32)
    pads[2:3, 0:ports] = port_cond[...]
    rows = pltpu.roll(pads[...], ports * lax.rem(j, pack), 1)
    info_send[...] = rows
    cell = rows[0:1].astype(I32) - 1
    valid = cell >= 0
    cell_row[...] = (
        iota((cells, LANES), 0) == jnp.where(valid, cell // ny, -1)
    ).astype(F32)
    cell_y[...] = (
        (iota((ny, LANES), 0) == jnp.where(valid, cell % ny, -1)).astype(F32).astype(BF16)
    )
    line_send[...] = jnp.zeros(line_send.shape, F32)
    line_send[0:1, :] = (line_far[...] + 1).astype(F32)
    line_send[1:2, :] = line_delay[...].astype(F32)
    line_send[2:3, :] = line_imped[...]
    for k in range(depth):
        line_send[3 + k : 4 + k, :] = hist_near[k]
        line_send[3 + depth + k : 4 + depth + k, :] = hist_far[k]

    def gather_cells(f):
        value = dot3(f.reshape(cells, ny), cell_y[...], ROWS)
        return jnp.sum(value * cell_row[...], axis=0, keepdims=True)

    loads[0].wait()
    info_send[4:5, :] = gather_cells(e[2])
    loads[1].wait()
    info_send[3:4, :] = gather_cells(gain[...])
    for z in range(cz):
        gain_send[z : z + 1, :] = gain[z, 0:1, :]
    info[j] = info_send[...]

    pl.semaphore_wait(barrier, nj - 1 + 2 * nj)
    for copy in info_copies:
        copy.start()
    when(has_above, [line_copy], "start")
    loads[2].wait()
    send_h(0)
    loads[3].wait()
    update_e()
    send_e(0)
    when(has_below, [gain_z], "start")
    when(has_left, [gain_x], "start")
    loads[4].wait()

    chunk = 32

    @pl.loop(0, block // chunk)
    def _(r):
        at = pl.ds(pl.multiple_of(r * chunk, chunk), chunk)
        x = inv[at, :]
        high = x.astype(BF16)
        inv2[at, :] = high
        inv2[pl.ds(pl.multiple_of(block + r * chunk, chunk), chunk), :] = (
            x - high.astype(F32)
        ).astype(BF16)

    when(has_below, [line_copy], "wait_recv")
    for copy in info_copies:
        copy.wait_recv()

    everyone = jnp.concatenate(
        [sum(info[t * pack + k] for k in range(pack)) for t in range(tiles)], 1
    )
    cell_all = everyone[0:1] - 1.0
    cond_all, gain_all = everyone[2:3], everyone[3:4]
    near_far = [line_near[...], line_info[0:1, :].astype(I32) - 1]
    index = jnp.concatenate([everyone[1:2].astype(I32) - 1, *near_far], 1)
    high = jnp.where(index >= 0, index // block, -1)
    low = jnp.where(index >= 0, index % block, -1)
    node_hi[...] = (iota(node_hi.shape, 0) == high).astype(F32)
    node_lo[...] = (iota(node_lo.shape, 0) == low).astype(F32).astype(BF16)

    delay = jnp.concatenate([line_delay[...].astype(F32), line_info[1:2, :]], 0)
    scale = -2.0 / jnp.concatenate([line_imped[...], line_info[2:3, :]], 0)
    past_a = [
        jnp.concatenate([hist_near[k], line_info[3 + k : 4 + k, :]], 0)
        for k in range(depth)
    ]
    past_b = [
        jnp.concatenate([hist_far[k], line_info[3 + depth + k : 4 + depth + k, :]], 0)
        for k in range(depth)
    ]
    waves_a, waves_b = [], []

    def incoming(n, waves, past):
        total = jnp.zeros((2, lines), F32)
        for k in range(1, depth + 1):
            value = waves[n - k] if n >= k else past[k - n - 1]
            total = jnp.where(delay == k, value, total)
        return total

    def sources(n, ez):
        in_a, in_b = incoming(n, waves_b, past_b), incoming(n, waves_a, past_a)
        return in_a, in_b, jnp.concatenate([cond_all * ez, -in_a[0:1], -in_b[1:2]], 1)

    def own_volts(src):
        totals = dot3(node_hi[...] * src, node_lo[...], COLS)[0:nj]

        @pl.loop(0, block // chunk)
        def _(r):
            at = pl.ds(pl.multiple_of(r * chunk, chunk), chunk)
            value = jnp.zeros((chunk, LANES), F32)
            for k in range(nodes // LANES):
                q, w = divmod(k * LANES, block)
                value = value + inv[at, k * LANES : (k + 1) * LANES] * totals[
                    q : q + 1, w : w + LANES
                ]
            acc[at, :] = value

        terms = jnp.concatenate(parts3(acc[...]), 1).astype(BF16)
        return dot(jnp.ones((16, 3 * LANES), BF16), terms, COLS)[0:1]

    key = cell_all + ((iota((1, np_), 1) // ports) * (cells * ny)).astype(F32)
    key_col = column(key)
    for t in range(0, np_, LANES):
        at = slice(t, t + LANES)
        same[:, at] = (key_col == key[:, at]).astype(F32) * cond_all[:, at]

    ez = everyone[4:5]
    in_a, in_b, src = sources(0, ez)
    v0 = sum3(dot(fold3(own_volts(src)), node_lo[...]))
    v0 = jnp.where(high == j, v0, 0.0)
    drive = lax.dot_general(
        jnp.broadcast_to(v0[:, 0:np_], (8, np_)), same[...], COLS,
        precision=lax.Precision.HIGHEST, preferred_element_type=F32,
    )[0:1]
    send_y(0, jnp.concatenate([gain_all * drive, v0[:, np_:]], 1))

    neighbour = info[right_id]
    cell_r = neighbour[0:1].astype(I32) - 1
    gain_r = neighbour[3:4]
    valid_r = (cell_r >= 0) & (lax.rem(cell_r // ny, cx) == 0) & has_right
    row_right[...] = (
        iota((cz, LANES), 0) == jnp.where(valid_r, cell_r // (cx * ny), -1)
    ).astype(F32)
    y_right[...] = (
        (iota((ny, LANES), 0) == jnp.where(valid_r, cell_r % ny, -1))
        .astype(F32)
        .astype(BF16)
    )

    def send_pre(n):
        value = gather_cells(e[2])
        side = dot3(hx_send[n - 1, 0], y_right[...], ROWS) * row_right[...]
        side = -gain_r * jnp.sum(side, axis=0, keepdims=True)
        for t in range(tiles):
            at = slice(t * LANES, (t + 1) * LANES)
            both = jnp.where(j // pack == t, value, 0.0)
            both = both + jnp.where(right_id // pack == t, side, 0.0)
            pre_send[n, :, at] = both
        pre[n, j] = pre_send[n]
        for copy in pre_copies(n):
            copy.start()

    send_pre(1)

    cond_col = column(cond_all)
    gain_col = column(gain_all)
    load, first = [], []
    for t in range(0, np_, LANES):
        hit = key_col == key[:, t : t + LANES]
        load.append(jnp.sum(jnp.where(hit, cond_col, 0.0), axis=0, keepdims=True))
        earlier = hit & (iota(hit.shape, 0) < iota(hit.shape, 1) + t)
        first.append(jnp.max(earlier.astype(F32), axis=0, keepdims=True))
    load = gain_all * jnp.concatenate(load, 1)
    first = 1.0 - jnp.concatenate(first, 1)

    @pl.loop(0, nodes // LANES)
    def _(r):
        at = pl.ds(pl.multiple_of(r * LANES, LANES), LANES)
        pick[at, :] = (iota((LANES, nt), 0) + r * LANES == index).astype(F32).astype(BF16)

    wide = 2 * LANES

    @pl.loop(0, nt // wide)
    def _(c):
        at = pl.ds(pl.multiple_of(c * wide, wide), wide)
        for half in range(2):
            rows = slice(half * block, (half + 1) * block)
            picked[rows, at] = dot(inv2[rows, :], pick[:, at]).astype(BF16)

    index_col = column(index.astype(F32))
    for w in range(0, block, LANES):
        node = (iota((nt, LANES), 1) + (w + j * block)).astype(F32)
        own_pick[:, w : w + LANES] = (index_col == node).astype(F32).astype(BF16)
    mixed = dot3(same[...], own_pick[0:np_, :], ROWS)
    for w in range(0, block, LANES):
        at = slice(w, w + LANES)
        value = mixed[:, at] * gain_col
        high_ = value.astype(BF16)
        left[0:np_, at] = high_
        left[np_ : 2 * np_, at] = (value - high_.astype(F32)).astype(BF16)
    left[2 * np_ :, :] = own_pick[np_:, :]
    upper = dot(left[...], picked[0:block, :])
    lower = dot(left[0:np_, :], picked[block:, :])
    value = upper[0:np_] + (upper[np_ : 2 * np_] + lower)
    high_ = value.astype(BF16)
    mat[0:np_, 0:nt] = high_
    mat[0:np_, nt:] = (value - high_.astype(F32)).astype(BF16)
    mat[np_:, 0:nt] = upper[2 * np_ :].astype(BF16)
    mat[np_:, nt:] = dot(left[2 * np_ :, :], picked[block:, :]).astype(BF16)

    def tile_of(x, device):
        out = x[:, 0:LANES]
        for t in range(1, tiles):
            out = jnp.where(device // pack == t, x[:, t * LANES : (t + 1) * LANES], out)
        return out

    when(has_above, [gain_z], "wait_recv")
    when(has_right, [gain_x], "wait_recv")
    at_x = slice(cx - 1, cx)

    for n in range(STEPS):
        slab, up, down = y_copies(n)
        for copy in slab:
            copy.wait_recv()
        when(has_below, up, "wait_recv")
        when(has_above, down, "wait_recv")
        total, v_below, v_above = y[n, 0], below[n, 0], above[n, 0]
        for k in range(1, nj):
            total = total + y[n, k]
            v_below = v_below + below[n, k]
            v_above = v_above + above[n, k]
        v_near = jnp.concatenate([total[:, np_ : np_ + lines], v_below], 0)
        v_far = jnp.concatenate([v_above, total[:, np_ + lines :]], 0)
        waves_a.append(scale * v_near - in_a)
        waves_b.append(scale * v_far - in_b)
        change = total[:, 0:np_] - load * ez
        if n + 1 < STEPS:
            for copy in pre_copies(n + 1):
                copy.wait_recv()
            ez = change + pre[n + 1, 0]
            for k in range(1, nj):
                ez = ez + pre[n + 1, k]
            in_a, in_b, src = sources(n + 1, ez)
            x = fold3(src)
            send_y(n + 1, sum3(dot(jnp.concatenate([x, x], 1), mat[...], COLS)))
        change = change * first
        drop = dot3(cell_row[...] * tile_of(change, j), cell_y[...], COLS)

        when(has_below, [down_z(n)], "wait_send")

        @pl.when(has_left)
        def _():
            up_x(n).wait_recv()
            for z in range(cz):
                g = gain[z, 0:1, :]
                e[1, z, 0:1, :] = e[1, z, 0:1, :] + g * hx[n, 1, z : z + 1, :]
                e[2, z, 0:1, :] = e[2, z, 0:1, :] - g * hx[n, 0, z : z + 1, :]

        @pl.when(has_below)
        def _():
            up_z(n).wait_recv()
            g = gain[0]
            e[0, 0] = e[0, 0] + g * hz[n, 1]
            e[1, 0] = e[1, 0] - g * hz[n, 0]

        e[2] = e[2] + drop.reshape(cz, cx, ny)
        when(has_above & has_left, [corner_down(n)], "wait_recv")
        when(has_below & has_right, [corner_up(n)], "wait_recv")

        @pl.when(has_above)
        def _():
            down_z(n).wait_recv()
            e_top[0] = ez_up[n, 0] + gain_top[...] * h[1, cz - 1]
            e_top[1] = ez_up[n, 1] - gain_top[...] * h[0, cz - 1]
            e_top[1, 0:1, :] = e_top[1, 0:1, :] + gain_top[0:1, :] * corner_a[n]
            up_z(n).wait_send()

        drop_right = dot3(row_right[...] * tile_of(change, right_id), y_right[...], COLS)
        update_h()

        @pl.when(has_right)
        def _():
            down_x(n).wait_recv()
            g = gain_right[...]
            face_y = ex[n, 0] + g * hx_send[n, 1]
            face_z = ex[n, 1] - g * hx_send[n, 0] + drop_right
            for z in range(cz):
                y_ = face_y[z : z + 1]
                if z == 0:
                    y_ = y_ - g[0:1] * corner_b[n]
                h[1, z, at_x, :] = h[1, z, at_x, :] + 0.5 * face_z[z : z + 1]
                h[2, z, at_x, :] = h[2, z, at_x, :] - 0.5 * y_

        if n + 1 < STEPS:
            send_h(n + 1)
            update_e()
            if n + 2 < STEPS:
                send_pre(n + 2)
            send_e(n + 1)
        if n + 2 == STEPS:
            volt_out[...] = own_volts(src)

    wave_out[0, 0:1, :] = waves_a[-1][0:1]
    wave_out[0, 1:2, :] = waves_b[-1][0:1]

    for copy in info_copies:
        copy.wait_send()
    when(has_above, [line_copy], "wait_send")
    when(has_below, [gain_z], "wait_send")
    when(has_left, [gain_x], "wait_send")
    for n in range(STEPS):
        slab, up, down = y_copies(n)
        for copy in slab:
            copy.wait_send()
        when(has_above, up, "wait_send")
        when(has_below, down, "wait_send")
        if n:
            for copy in pre_copies(n):
                copy.wait_send()
        when(has_right, [up_x(n)], "wait_send")
        when(has_left, [down_x(n)], "wait_send")
        when(has_below & has_right, [corner_down(n)], "wait_send")
        when(has_above & has_left, [corner_up(n)], "wait_send")


def local(*args):
    e_field, inverse = args[0], args[7]
    nj = lax.axis_size("fxy")
    _, cz, cx, ny = e_field.shape
    _, block, nodes = inverse.shape
    ports, lines = args[4].shape[1], args[8].shape[1]
    args = [*args[:12], *(a.transpose(1, 0, 2) for a in args[12:])]
    depth = args[12].shape[0]
    vmem = pl.BlockSpec(memory_space=pltpu.VMEM)
    hbm = pl.BlockSpec(memory_space=pltpu.HBM)
    small = [a for i, a in enumerate(args) if i not in (0, 1, 2, 3, 7)]
    rows = -(-nj // 16) * 16
    np_ = nj * ports
    nt = np_ + 2 * lines
    line_rows = -(-(3 + 2 * depth) // 8) * 8
    dma = pltpu.SemaphoreType.DMA
    v = pltpu.VMEM
    e, h, volt, wave = pl.pallas_call(
        kernel,
        out_shape=(
            v(e_field.shape, F32),
            v(e_field.shape, F32),
            v((1, block), F32),
            v((1, 2, lines), F32),
        ),
        in_specs=[hbm] * len(args),
        out_specs=(vmem,) * 4,
        scratch_shapes=[
            *[v(a.shape, a.dtype) for a in small],
            v((2, cx, ny), F32),
            v((cz, cx, ny), F32),
            v((cz, cx, ny), F32),
            v((cx, ny), F32),
            v((cz, ny), F32),
            v((cz, ny), F32),
            v((block, nodes), F32),
            v((2 * block, nodes), BF16),
            v((nodes, nt), BF16),
            v((2 * block, nt), BF16),
            v((nt, block), BF16),
            v((np_, np_), F32),
            v((2 * np_ + 2 * lines, block), BF16),
            v((nt, 2 * nt), BF16),
            v((cz * cx, LANES), F32),
            v((ny, LANES), BF16),
            v((cz, LANES), F32),
            v((ny, LANES), BF16),
            v((rows, nt), F32),
            v((block, nt), BF16),
            v((8, LANES), F32),
            v((8, LANES), F32),
            v((nj, 8, LANES), F32),
            v((line_rows, lines), F32),
            v((line_rows, lines), F32),
            v((STEPS, 1, np_), F32),
            v((STEPS, nj, 1, np_), F32),
            v((STEPS, 1, nt), F32),
            v((STEPS, nj, 1, nt), F32),
            v((STEPS, nj, 1, lines), F32),
            v((STEPS, nj, 1, lines), F32),
            v((STEPS, 2, cx, ny), F32),
            v((STEPS, 2, cx, ny), F32),
            v((STEPS, 2, cz, ny), F32),
            v((STEPS, 2, cz, ny), F32),
            v((STEPS, 2, cz, ny), F32),
            v((STEPS, 2, cz, ny), F32),
            v((STEPS, 2, 1, ny), F32),
            v((STEPS, 1, ny), F32),
            v((STEPS, 1, ny), F32),
            v((block, LANES), F32),
            dma((5 + len(small),)),
            dma((7, STEPS)),
            dma((7, STEPS)),
            dma((nj - 1,)),
            dma((nj - 1,)),
            dma((STEPS, nj - 1)),
            dma((STEPS, nj - 1)),
            dma((STEPS, nj - 1)),
            dma((STEPS, nj - 1)),
            dma((STEPS, nj)),
            dma((STEPS, nj)),
            dma((STEPS, nj)),
            dma((STEPS, nj)),
        ],
        compiler_params=pltpu.CompilerParams(
            collective_id=0, has_side_effects=True, vmem_limit_bytes=61 * 1024 * 1024
        ),
    )(*args)
    outs = [pltpu.with_memory_space_constraint(x, pltpu.VMEM) for x in (e, h, volt, wave)]
    return pl.pallas_call(
        store,
        out_shape=[jax.ShapeDtypeStruct(x.shape, F32) for x in outs],
        in_specs=[vmem] * 4,
        out_specs=[hbm] * 4,
        scratch_shapes=[dma((4,))],
    )(*outs)


def store(e, h, volt, wave, e_out, h_out, volt_out, wave_out, sem):
    pairs = ((e, e_out), (h, h_out), (volt, volt_out), (wave, wave_out))
    copies = [pltpu.make_async_copy(a, b, sem.at[k]) for k, (a, b) in enumerate(pairs)]
    for copy in copies:
        copy.start()
    for copy in copies:
        copy.wait()


def solution(mesh):
    placed = (
        P(None, "fz", "fxy", None),
        P(None, "fz", "fxy", None),
        P("fz", "fxy", None),
        P("fz", "fxy", None),
        P("fz", "fxy"),
        P("fz", "fxy"),
        P("fz", "fxy"),
        P("fz", "fxy", None),
        P("fz", None),
        P("fz", None),
        P("fz", None),
        P("fz", None),
        P("fz", None, None),
        P("fz", None, None),
    )
    return jax.shard_map(
        local,
        mesh=mesh,
        in_specs=placed,
        out_specs=(
            P(None, "fz", "fxy", None),
            P(None, "fz", "fxy", None),
            P("fz", "fxy"),
            P("fz", None, None),
        ),
        check_vma=False,
    )
```

```python
import jax
import jax.numpy as jnp
from jax import lax
from jax.experimental import pallas as pl
from jax.experimental.pallas import tpu as pltpu
from jax.sharding import PartitionSpec as P

STEPS = 4
LANES = 128
F32 = jnp.float32
BF16 = jnp.bfloat16
I32 = jnp.int32
MESH = pl.DeviceIdType.MESH
ROWS = (((1,), (0,)), ((), ()))
COLS = (((1,), (1,)), ((), ()))


def iota(shape, dim):
    return lax.broadcasted_iota(I32, shape, dim)


def parts3(x):
    a = x.astype(BF16).astype(F32)
    r = x - a
    b = r.astype(BF16).astype(F32)
    return a, b, r - b


def dot(x, y, dims=ROWS):
    return lax.dot_general(x, y, dims, preferred_element_type=F32)


def dot3(x, onehot, dims):
    rows = x.shape[0]
    parts = list(parts3(x))
    pad = -3 * rows % 16
    if pad:
        parts.append(jnp.zeros((pad, x.shape[1]), F32))
    y = dot(jnp.concatenate(parts, 0).astype(BF16), onehot, dims)
    return y[:rows] + y[rows : 2 * rows] + y[2 * rows : 3 * rows]


def fold3(x):
    a, b, c = parts3(jnp.broadcast_to(x, (16, x.shape[1])))
    r = iota(a.shape, 0)
    x = jnp.where(r == 0, a, jnp.where(r == 1, b, jnp.where(r == 2, c, 0.0)))
    return x.astype(BF16)


def sum3(y):
    return y[0:1] + y[1:2] + y[2:3]


def column(row):
    return jnp.concatenate(
        [
            jnp.broadcast_to(row[:, t : t + LANES], (LANES, LANES)).T
            for t in range(0, row.shape[1], LANES)
        ],
        0,
    )


def kernel(
    e_in, h_in, decay_in, gain_in, port_cell_in, port_node_in, port_cond_in, inv_in,
    line_near_in, line_far_in, line_delay_in, line_imped_in, hist_near_in, hist_far_in,
    e, h, volt_out, wave_out,
    port_cell, port_node, port_cond, line_near, line_far, line_delay, line_imped,
    hist_near, hist_far,
    e_top, decay, gain, gain_top, gain_send, gain_right, inv, inv2, pick, picked, own_pick,
    same, left, mat, cell_row, cell_y, row_right, y_right, node_hi, node_lo, pads,
    info_send, info, line_send, line_info, pre_send, pre, y_send, y, below, above,
    hz, ez_up, hx_send, hx, ex_send, ex, corner_send, corner_a, corner_b, acc,
    load_sem, face_ss, face_rs, info_ss, info_rs, pre_ss, pre_rs, y_ss, y_rs,
    up_ss, up_rs, down_ss, down_rs,
):
    s, j = lax.axis_index("fz"), lax.axis_index("fxy")
    ns, nj = lax.axis_size("fz"), lax.axis_size("fxy")
    above_id, below_id = lax.rem(s + 1, ns), lax.rem(s + ns - 1, ns)
    right_id, left_id = lax.rem(j + 1, nj), lax.rem(j + nj - 1, nj)
    has_above, has_below = s < ns - 1, s > 0
    has_right, has_left = j < nj - 1, j > 0
    _, cz, cx, ny = e_in.shape
    cells = cz * cx
    block, nodes = inv_in.shape[1:]
    ports = port_cell_in.shape[1]
    lines = line_near_in.shape[1]
    depth = hist_near_in.shape[0]
    pack = LANES // ports
    tiles = nj // pack
    np_ = nj * ports
    nt = np_ + 2 * lines

    loads = [
        pltpu.make_async_copy(e_in, e, load_sem.at[0]),
        pltpu.make_async_copy(gain_in, gain, load_sem.at[1]),
        pltpu.make_async_copy(h_in, h, load_sem.at[2]),
        pltpu.make_async_copy(decay_in, decay, load_sem.at[3]),
        pltpu.make_async_copy(inv_in.at[0], inv, load_sem.at[4]),
    ]
    small = (
        (port_cell_in, port_cell), (port_node_in, port_node), (port_cond_in, port_cond),
        (line_near_in, line_near), (line_far_in, line_far), (line_delay_in, line_delay),
        (line_imped_in, line_imped), (hist_near_in, hist_near), (hist_far_in, hist_far),
    )
    small = [
        pltpu.make_async_copy(src, dst, load_sem.at[5 + k])
        for k, (src, dst) in enumerate(small)
    ]
    for copy in small + loads:
        copy.start()

    e_top[...] = jnp.zeros(e_top.shape, F32)
    below[...] = jnp.zeros(below.shape, F32)
    above[...] = jnp.zeros(above.shape, F32)
    corner_a[...] = jnp.zeros(corner_a.shape, F32)
    corner_b[...] = jnp.zeros(corner_b.shape, F32)
    line_info[...] = (iota(line_info.shape, 0) == 2).astype(F32)

    barrier = pltpu.get_barrier_semaphore()
    for other in (above_id, below_id):
        for d in range(nj):
            pl.semaphore_signal(
                barrier, inc=1, device_id={"fz": other, "fxy": lax.rem(j + d, nj)},
                device_id_type=MESH,
            )
    for d in range(1, nj):
        pl.semaphore_signal(
            barrier, inc=1, device_id={"fxy": lax.rem(j + d, nj)}, device_id_type=MESH
        )

    def remote(src, dst, ss, rs, **where):
        return pltpu.make_async_remote_copy(
            src_ref=src, dst_ref=dst, send_sem=ss, recv_sem=rs,
            device_id=where, device_id_type=MESH,
        )

    def face(kind, n, src, dst, **where):
        return remote(src, dst, face_ss.at[kind, n], face_rs.at[kind, n], **where)

    def when(cond, copies, act):
        @pl.when(cond)
        def _():
            for copy in copies:
                getattr(copy, act)()

    def up_z(n):
        return face(0, n, h.at[0:2, cz - 1], hz.at[n], fz=above_id)

    def up_x(n):
        return face(1, n, hx_send.at[n], hx.at[n], fxy=right_id)

    def down_z(n):
        return face(2, n, e.at[0:2, 0], ez_up.at[n], fz=below_id)

    def down_x(n):
        return face(3, n, ex_send.at[n], ex.at[n], fxy=left_id)

    def corner_down(n):
        return face(4, n, corner_send.at[n, 0], corner_a.at[n], fz=below_id, fxy=right_id)

    def corner_up(n):
        return face(5, n, corner_send.at[n, 1], corner_b.at[n], fz=above_id, fxy=left_id)

    line_copy = face(6, 0, line_send, line_info, fz=above_id)
    gain_z = face(6, 1, gain.at[0], gain_top, fz=below_id)
    gain_x = face(6, 2, gain_send, gain_right, fxy=left_id)

    def spread(src, dst, ss, rs):
        return [
            remote(src, dst, ss.at[d - 1], rs.at[d - 1], fxy=lax.rem(j + d, nj))
            for d in range(1, nj)
        ]

    def spread_z(src, dst, ss, rs, to):
        return [
            remote(src, dst, ss.at[d], rs.at[d], fz=to, fxy=lax.rem(j + d, nj))
            for d in range(nj)
        ]

    info_copies = spread(info_send, info.at[j], info_ss, info_rs)

    def pre_copies(n):
        return spread(pre_send.at[n], pre.at[n, j], pre_ss.at[n], pre_rs.at[n])

    def y_copies(n):
        return (
            spread(y_send.at[n], y.at[n, j], y_ss.at[n], y_rs.at[n]),
            spread_z(
                y_send.at[n, :, np_ : np_ + lines], below.at[n, j],
                up_ss.at[n], up_rs.at[n], above_id,
            ),
            spread_z(
                y_send.at[n, :, np_ + lines : nt], above.at[n, j],
                down_ss.at[n], down_rs.at[n], below_id,
            ),
        )

    def send_y(n, value):
        y_send[n] = value
        y[n, j] = value
        slab, up, down = y_copies(n)
        when(has_above, up, "start")
        when(has_below, down, "start")
        for copy in slab:
            copy.start()

    def send_h(n):
        for c in range(2):
            for z in range(cz):
                hx_send[n, c, z : z + 1, :] = h[1 + c, z, cx - 1 : cx, :]
        corner_send[n, 0] = h[2, 0, cx - 1 : cx, :]
        corner_send[n, 1] = h[0, cz - 1, 0:1, :]
        when(has_above, [up_z(n)], "start")
        when(has_right, [up_x(n)], "start")
        when(has_below & has_right, [corner_down(n)], "start")
        when(has_above & has_left, [corner_up(n)], "start")

    def send_e(n):
        for c in range(2):
            for z in range(cz):
                ex_send[n, c, z : z + 1, :] = e[1 + c, z, 0:1, :]
        when(has_below, [down_z(n)], "start")
        when(has_left, [down_x(n)], "start")

    lane = iota((cx, ny), 1)
    sub = iota((cx, ny), 0)

    def update_e():
        def plane(z, lower):
            hx_, hy_, hz_ = (h[c, z] for c in range(3))
            dx, dy = hx_, hy_
            if lower is not None:
                dx, dy = hx_ - h[0, lower], hy_ - h[1, lower]

            def by(f):
                return f - jnp.where(lane == 0, 0.0, pltpu.roll(f, 1, 1))

            def bx(f):
                return f - jnp.where(sub == 0, 0.0, pltpu.roll(f, 1, 0))

            g, q = gain[z], decay[z]
            e[0, z] = q * e[0, z] + g * (by(hz_) - dy)
            e[1, z] = q * e[1, z] + g * (dx - bx(hz_))
            e[2, z] = q * e[2, z] + g * (bx(hy_) - by(hx_))

        plane(0, None)

        @pl.loop(1, cz, unroll=True)
        def _(z):
            plane(z, z - 1)

    def update_h():
        def plane(z, ux, uy):
            ex_, ey_, ez_ = (e[c, z] for c in range(3))

            def dy(f):
                return jnp.where(lane == ny - 1, 0.0, pltpu.roll(f, ny - 1, 1)) - f

            def dx(f):
                return jnp.where(sub == cx - 1, 0.0, pltpu.roll(f, cx - 1, 0)) - f

            h[0, z] = h[0, z] - 0.5 * (dy(ez_) - (uy - ey_))
            h[1, z] = h[1, z] - 0.5 * ((ux - ex_) - dx(ez_))
            h[2, z] = h[2, z] - 0.5 * (dx(ey_) - dy(ex_))

        @pl.loop(0, cz - 1, unroll=True)
        def _(z):
            plane(z, e[0, z + 1], e[1, z + 1])

        plane(cz - 1, e_top[0], e_top[1])

    for copy in small:
        copy.wait()

    pads[...] = jnp.zeros(pads.shape, F32)
    pads[0:1, 0:ports] = (port_cell[...] + 1).astype(F32)
    pads[1:2, 0:ports] = (port_node[...] + 1).astype(F32)
    pads[2:3, 0:ports] = port_cond[...]
    rows = pltpu.roll(pads[...], ports * lax.rem(j, pack), 1)
    info_send[...] = rows
    cell = rows[0:1].astype(I32) - 1
    valid = cell >= 0
    cell_row[...] = (
        iota((cells, LANES), 0) == jnp.where(valid, cell // ny, -1)
    ).astype(F32)
    cell_y[...] = (
        (iota((ny, LANES), 0) == jnp.where(valid, cell % ny, -1)).astype(F32).astype(BF16)
    )
    line_send[...] = jnp.zeros(line_send.shape, F32)
    line_send[0:1, :] = (line_far[...] + 1).astype(F32)
    line_send[1:2, :] = line_delay[...].astype(F32)
    line_send[2:3, :] = line_imped[...]
    for k in range(depth):
        line_send[3 + k : 4 + k, :] = hist_near[k]
        line_send[3 + depth + k : 4 + depth + k, :] = hist_far[k]

    def gather_cells(f):
        value = dot3(f.reshape(cells, ny), cell_y[...], ROWS)
        return jnp.sum(value * cell_row[...], axis=0, keepdims=True)

    loads[0].wait()
    info_send[4:5, :] = gather_cells(e[2])
    loads[1].wait()
    info_send[3:4, :] = gather_cells(gain[...])
    for z in range(cz):
        gain_send[z : z + 1, :] = gain[z, 0:1, :]
    info[j] = info_send[...]

    pl.semaphore_wait(barrier, nj - 1 + 2 * nj)
    for copy in info_copies:
        copy.start()
    when(has_above, [line_copy], "start")
    loads[2].wait()
    send_h(0)
    loads[3].wait()
    update_e()
    send_e(0)
    when(has_below, [gain_z], "start")
    when(has_left, [gain_x], "start")
    loads[4].wait()

    chunk = 32

    @pl.loop(0, block // chunk)
    def _(r):
        at = pl.ds(pl.multiple_of(r * chunk, chunk), chunk)
        x = inv[at, :]
        high = x.astype(BF16)
        inv2[at, :] = high
        inv2[pl.ds(pl.multiple_of(block + r * chunk, chunk), chunk), :] = (
            x - high.astype(F32)
        ).astype(BF16)

    when(has_below, [line_copy], "wait_recv")
    for copy in info_copies:
        copy.wait_recv()

    everyone = jnp.concatenate(
        [sum(info[t * pack + k] for k in range(pack)) for t in range(tiles)], 1
    )
    cell_all = everyone[0:1] - 1.0
    cond_all, gain_all = everyone[2:3], everyone[3:4]
    near_far = [line_near[...], line_info[0:1, :].astype(I32) - 1]
    index = jnp.concatenate([everyone[1:2].astype(I32) - 1, *near_far], 1)
    high = jnp.where(index >= 0, index // block, -1)
    low = jnp.where(index >= 0, index % block, -1)
    node_hi[...] = (iota(node_hi.shape, 0) == high).astype(F32)
    node_lo[...] = (iota(node_lo.shape, 0) == low).astype(F32).astype(BF16)

    delay = jnp.concatenate([line_delay[...].astype(F32), line_info[1:2, :]], 0)
    scale = -2.0 / jnp.concatenate([line_imped[...], line_info[2:3, :]], 0)
    past_a = [
        jnp.concatenate([hist_near[k], line_info[3 + k : 4 + k, :]], 0)
        for k in range(depth)
    ]
    past_b = [
        jnp.concatenate([hist_far[k], line_info[3 + depth + k : 4 + depth + k, :]], 0)
        for k in range(depth)
    ]
    waves_a, waves_b = [], []

    def incoming(n, waves, past):
        total = jnp.zeros((2, lines), F32)
        for k in range(1, depth + 1):
            value = waves[n - k] if n >= k else past[k - n - 1]
            total = jnp.where(delay == k, value, total)
        return total

    def sources(n, ez):
        in_a, in_b = incoming(n, waves_b, past_b), incoming(n, waves_a, past_a)
        return in_a, in_b, jnp.concatenate([cond_all * ez, -in_a[0:1], -in_b[1:2]], 1)

    def own_volts(src):
        totals = dot3(node_hi[...] * src, node_lo[...], COLS)[0:nj]

        @pl.loop(0, block // chunk)
        def _(r):
            at = pl.ds(pl.multiple_of(r * chunk, chunk), chunk)
            value = jnp.zeros((chunk, LANES), F32)
            for k in range(nodes // LANES):
                q, w = divmod(k * LANES, block)
                value = value + inv[at, k * LANES : (k + 1) * LANES] * totals[
                    q : q + 1, w : w + LANES
                ]
            acc[at, :] = value

        terms = jnp.concatenate(parts3(acc[...]), 1).astype(BF16)
        return dot(jnp.ones((16, 3 * LANES), BF16), terms, COLS)[0:1]

    key = cell_all + ((iota((1, np_), 1) // ports) * (cells * ny)).astype(F32)
    key_col = column(key)
    for t in range(0, np_, LANES):
        at = slice(t, t + LANES)
        same[:, at] = (key_col == key[:, at]).astype(F32) * cond_all[:, at]

    ez = everyone[4:5]
    in_a, in_b, src = sources(0, ez)
    v0 = sum3(dot(fold3(own_volts(src)), node_lo[...]))
    v0 = jnp.where(high == j, v0, 0.0)
    drive = lax.dot_general(
        jnp.broadcast_to(v0[:, 0:np_], (8, np_)), same[...], COLS,
        precision=lax.Precision.HIGHEST, preferred_element_type=F32,
    )[0:1]
    send_y(0, jnp.concatenate([gain_all * drive, v0[:, np_:]], 1))

    neighbour = info[right_id]
    cell_r = neighbour[0:1].astype(I32) - 1
    gain_r = neighbour[3:4]
    valid_r = (cell_r >= 0) & (lax.rem(cell_r // ny, cx) == 0) & has_right
    row_right[...] = (
        iota((cz, LANES), 0) == jnp.where(valid_r, cell_r // (cx * ny), -1)
    ).astype(F32)
    y_right[...] = (
        (iota((ny, LANES), 0) == jnp.where(valid_r, cell_r % ny, -1))
        .astype(F32)
        .astype(BF16)
    )

    def send_pre(n):
        value = gather_cells(e[2])
        side = dot3(hx_send[n - 1, 0], y_right[...], ROWS) * row_right[...]
        side = -gain_r * jnp.sum(side, axis=0, keepdims=True)
        for t in range(tiles):
            at = slice(t * LANES, (t + 1) * LANES)
            both = jnp.where(j // pack == t, value, 0.0)
            both = both + jnp.where(right_id // pack == t, side, 0.0)
            pre_send[n, :, at] = both
        pre[n, j] = pre_send[n]
        for copy in pre_copies(n):
            copy.start()

    send_pre(1)

    cond_col = column(cond_all)
    gain_col = column(gain_all)
    load, first = [], []
    for t in range(0, np_, LANES):
        hit = key_col == key[:, t : t + LANES]
        load.append(jnp.sum(jnp.where(hit, cond_col, 0.0), axis=0, keepdims=True))
        earlier = hit & (iota(hit.shape, 0) < iota(hit.shape, 1) + t)
        first.append(jnp.max(earlier.astype(F32), axis=0, keepdims=True))
    load = gain_all * jnp.concatenate(load, 1)
    first = 1.0 - jnp.concatenate(first, 1)

    @pl.loop(0, nodes // LANES)
    def _(r):
        at = pl.ds(pl.multiple_of(r * LANES, LANES), LANES)
        pick[at, :] = (iota((LANES, nt), 0) + r * LANES == index).astype(F32).astype(BF16)

    wide = 2 * LANES

    @pl.loop(0, nt // wide)
    def _(c):
        at = pl.ds(pl.multiple_of(c * wide, wide), wide)
        for half in range(2):
            rows = slice(half * block, (half + 1) * block)
            picked[rows, at] = dot(inv2[rows, :], pick[:, at]).astype(BF16)

    index_col = column(index.astype(F32))
    for w in range(0, block, LANES):
        node = (iota((nt, LANES), 1) + (w + j * block)).astype(F32)
        own_pick[:, w : w + LANES] = (index_col == node).astype(F32).astype(BF16)
    mixed = dot3(same[...], own_pick[0:np_, :], ROWS)
    for w in range(0, block, LANES):
        at = slice(w, w + LANES)
        value = mixed[:, at] * gain_col
        high_ = value.astype(BF16)
        left[0:np_, at] = high_
        left[np_ : 2 * np_, at] = (value - high_.astype(F32)).astype(BF16)
    left[2 * np_ :, :] = own_pick[np_:, :]
    upper = dot(left[...], picked[0:block, :])
    lower = dot(left[0:np_, :], picked[block:, :])
    value = upper[0:np_] + (upper[np_ : 2 * np_] + lower)
    high_ = value.astype(BF16)
    mat[0:np_, 0:nt] = high_
    mat[0:np_, nt:] = (value - high_.astype(F32)).astype(BF16)
    mat[np_:, 0:nt] = upper[2 * np_ :].astype(BF16)
    mat[np_:, nt:] = dot(left[2 * np_ :, :], picked[block:, :]).astype(BF16)

    def tile_of(x, device):
        out = x[:, 0:LANES]
        for t in range(1, tiles):
            out = jnp.where(device // pack == t, x[:, t * LANES : (t + 1) * LANES], out)
        return out

    when(has_above, [gain_z], "wait_recv")
    when(has_right, [gain_x], "wait_recv")
    at_x = slice(cx - 1, cx)

    for n in range(STEPS):
        slab, up, down = y_copies(n)
        for copy in slab:
            copy.wait_recv()
        when(has_below, up, "wait_recv")
        when(has_above, down, "wait_recv")
        total, v_below, v_above = y[n, 0], below[n, 0], above[n, 0]
        for k in range(1, nj):
            total = total + y[n, k]
            v_below = v_below + below[n, k]
            v_above = v_above + above[n, k]
        v_near = jnp.concatenate([total[:, np_ : np_ + lines], v_below], 0)
        v_far = jnp.concatenate([v_above, total[:, np_ + lines :]], 0)
        waves_a.append(scale * v_near - in_a)
        waves_b.append(scale * v_far - in_b)
        change = total[:, 0:np_] - load * ez
        if n + 1 < STEPS:
            for copy in pre_copies(n + 1):
                copy.wait_recv()
            ez = change + pre[n + 1, 0]
            for k in range(1, nj):
                ez = ez + pre[n + 1, k]
            in_a, in_b, src = sources(n + 1, ez)
            x = fold3(src)
            send_y(n + 1, sum3(dot(jnp.concatenate([x, x], 1), mat[...], COLS)))
        change = change * first
        drop = dot3(cell_row[...] * tile_of(change, j), cell_y[...], COLS)

        when(has_below, [down_z(n)], "wait_send")

        @pl.when(has_left)
        def _():
            up_x(n).wait_recv()
            for z in range(cz):
                g = gain[z, 0:1, :]
                e[1, z, 0:1, :] = e[1, z, 0:1, :] + g * hx[n, 1, z : z + 1, :]
                e[2, z, 0:1, :] = e[2, z, 0:1, :] - g * hx[n, 0, z : z + 1, :]

        @pl.when(has_below)
        def _():
            up_z(n).wait_recv()
            g = gain[0]
            e[0, 0] = e[0, 0] + g * hz[n, 1]
            e[1, 0] = e[1, 0] - g * hz[n, 0]

        e[2] = e[2] + drop.reshape(cz, cx, ny)
        when(has_above & has_left, [corner_down(n)], "wait_recv")
        when(has_below & has_right, [corner_up(n)], "wait_recv")

        @pl.when(has_above)
        def _():
            down_z(n).wait_recv()
            e_top[0] = ez_up[n, 0] + gain_top[...] * h[1, cz - 1]
            e_top[1] = ez_up[n, 1] - gain_top[...] * h[0, cz - 1]
            e_top[1, 0:1, :] = e_top[1, 0:1, :] + gain_top[0:1, :] * corner_a[n]
            up_z(n).wait_send()

        drop_right = dot3(row_right[...] * tile_of(change, right_id), y_right[...], COLS)
        update_h()

        @pl.when(has_right)
        def _():
            down_x(n).wait_recv()
            g = gain_right[...]
            face_y = ex[n, 0] + g * hx_send[n, 1]
            face_z = ex[n, 1] - g * hx_send[n, 0] + drop_right
            for z in range(cz):
                y_ = face_y[z : z + 1]
                if z == 0:
                    y_ = y_ - g[0:1] * corner_b[n]
                h[1, z, at_x, :] = h[1, z, at_x, :] + 0.5 * face_z[z : z + 1]
                h[2, z, at_x, :] = h[2, z, at_x, :] - 0.5 * y_

        if n + 1 < STEPS:
            send_h(n + 1)
            update_e()
            if n + 2 < STEPS:
                send_pre(n + 2)
            send_e(n + 1)
        if n + 2 == STEPS:
            volt_out[...] = own_volts(src)

    wave_out[0, 0:1, :] = waves_a[-1][0:1]
    wave_out[0, 1:2, :] = waves_b[-1][0:1]

    for copy in info_copies:
        copy.wait_send()
    when(has_above, [line_copy], "wait_send")
    when(has_below, [gain_z], "wait_send")
    when(has_left, [gain_x], "wait_send")
    for n in range(STEPS):
        slab, up, down = y_copies(n)
        for copy in slab:
            copy.wait_send()
        when(has_above, up, "wait_send")
        when(has_below, down, "wait_send")
        if n:
            for copy in pre_copies(n):
                copy.wait_send()
        when(has_right, [up_x(n)], "wait_send")
        when(has_left, [down_x(n)], "wait_send")
        when(has_below & has_right, [corner_down(n)], "wait_send")
        when(has_above & has_left, [corner_up(n)], "wait_send")


def local(*args):
    e_field, inverse = args[0], args[7]
    nj = lax.axis_size("fxy")
    _, cz, cx, ny = e_field.shape
    _, block, nodes = inverse.shape
    ports, lines = args[4].shape[1], args[8].shape[1]
    args = [*args[:12], *(a.transpose(1, 0, 2) for a in args[12:])]
    depth = args[12].shape[0]
    vmem = pl.BlockSpec(memory_space=pltpu.VMEM)
    hbm = pl.BlockSpec(memory_space=pltpu.HBM)
    small = [a for i, a in enumerate(args) if i not in (0, 1, 2, 3, 7)]
    rows = -(-nj // 16) * 16
    np_ = nj * ports
    nt = np_ + 2 * lines
    line_rows = -(-(3 + 2 * depth) // 8) * 8
    dma = pltpu.SemaphoreType.DMA
    v = pltpu.VMEM
    e, h, volt, wave = pl.pallas_call(
        kernel,
        out_shape=(
            v(e_field.shape, F32),
            v(e_field.shape, F32),
            v((1, block), F32),
            v((1, 2, lines), F32),
        ),
        in_specs=[hbm] * len(args),
        out_specs=(vmem,) * 4,
        scratch_shapes=[
            *[v(a.shape, a.dtype) for a in small],
            v((2, cx, ny), F32),
            v((cz, cx, ny), F32),
            v((cz, cx, ny), F32),
            v((cx, ny), F32),
            v((cz, ny), F32),
            v((cz, ny), F32),
            v((block, nodes), F32),
            v((2 * block, nodes), BF16),
            v((nodes, nt), BF16),
            v((2 * block, nt), BF16),
            v((nt, block), BF16),
            v((np_, np_), F32),
            v((2 * np_ + 2 * lines, block), BF16),
            v((nt, 2 * nt), BF16),
            v((cz * cx, LANES), F32),
            v((ny, LANES), BF16),
            v((cz, LANES), F32),
            v((ny, LANES), BF16),
            v((rows, nt), F32),
            v((block, nt), BF16),
            v((8, LANES), F32),
            v((8, LANES), F32),
            v((nj, 8, LANES), F32),
            v((line_rows, lines), F32),
            v((line_rows, lines), F32),
            v((STEPS, 1, np_), F32),
            v((STEPS, nj, 1, np_), F32),
            v((STEPS, 1, nt), F32),
            v((STEPS, nj, 1, nt), F32),
            v((STEPS, nj, 1, lines), F32),
            v((STEPS, nj, 1, lines), F32),
            v((STEPS, 2, cx, ny), F32),
            v((STEPS, 2, cx, ny), F32),
            v((STEPS, 2, cz, ny), F32),
            v((STEPS, 2, cz, ny), F32),
            v((STEPS, 2, cz, ny), F32),
            v((STEPS, 2, cz, ny), F32),
            v((STEPS, 2, 1, ny), F32),
            v((STEPS, 1, ny), F32),
            v((STEPS, 1, ny), F32),
            v((block, LANES), F32),
            dma((5 + len(small),)),
            dma((7, STEPS)),
            dma((7, STEPS)),
            dma((nj - 1,)),
            dma((nj - 1,)),
            dma((STEPS, nj - 1)),
            dma((STEPS, nj - 1)),
            dma((STEPS, nj - 1)),
            dma((STEPS, nj - 1)),
            dma((STEPS, nj)),
            dma((STEPS, nj)),
            dma((STEPS, nj)),
            dma((STEPS, nj)),
        ],
        compiler_params=pltpu.CompilerParams(
            collective_id=0, has_side_effects=True, vmem_limit_bytes=61 * 1024 * 1024
        ),
    )(*args)
    outs = [pltpu.with_memory_space_constraint(x, pltpu.VMEM) for x in (e, h, volt, wave)]
    return pl.pallas_call(
        store,
        out_shape=[jax.ShapeDtypeStruct(x.shape, F32) for x in outs],
        in_specs=[vmem] * 4,
        out_specs=[hbm] * 4,
        scratch_shapes=[dma((4,))],
    )(*outs)


def store(e, h, volt, wave, e_out, h_out, volt_out, wave_out, sem):
    pairs = ((e, e_out), (h, h_out), (volt, volt_out), (wave, wave_out))
    copies = [pltpu.make_async_copy(a, b, sem.at[k]) for k, (a, b) in enumerate(pairs)]
    for copy in copies:
        copy.start()
    for copy in copies:
        copy.wait()


def solution(mesh):
    placed = (
        P(None, "fz", "fxy", None),
        P(None, "fz", "fxy", None),
        P("fz", "fxy", None),
        P("fz", "fxy", None),
        P("fz", "fxy"),
        P("fz", "fxy"),
        P("fz", "fxy"),
        P("fz", "fxy", None),
        P("fz", None),
        P("fz", None),
        P("fz", None),
        P("fz", None),
        P("fz", None, None),
        P("fz", None, None),
    )
    return jax.shard_map(
        local,
        mesh=mesh,
        in_specs=placed,
        out_specs=(
            P(None, "fz", "fxy", None),
            P(None, "fz", "fxy", None),
            P("fz", "fxy"),
            P("fz", None, None),
        ),
        check_vma=False,
    )
```

```python
import jax
import jax.numpy as jnp
from jax import lax
from jax.experimental import pallas as pl
from jax.experimental.pallas import tpu as pltpu
from jax.sharding import PartitionSpec as P

STEPS = 4
LANES = 128
F32 = jnp.float32
BF16 = jnp.bfloat16
I32 = jnp.int32
MESH = pl.DeviceIdType.MESH
ROWS = (((1,), (0,)), ((), ()))
COLS = (((1,), (1,)), ((), ()))


def iota(shape, dim):
    return lax.broadcasted_iota(I32, shape, dim)


def parts3(x):
    a = x.astype(BF16).astype(F32)
    r = x - a
    b = r.astype(BF16).astype(F32)
    return a, b, r - b


def dot(x, y, dims=ROWS):
    return lax.dot_general(x, y, dims, preferred_element_type=F32)


def dot3(x, onehot, dims):
    rows = x.shape[0]
    parts = list(parts3(x))
    pad = -3 * rows % 16
    if pad:
        parts.append(jnp.zeros((pad, x.shape[1]), F32))
    y = dot(jnp.concatenate(parts, 0).astype(BF16), onehot, dims)
    return y[:rows] + y[rows : 2 * rows] + y[2 * rows : 3 * rows]


def fold3(x):
    a, b, c = parts3(jnp.broadcast_to(x, (16, x.shape[1])))
    r = iota(a.shape, 0)
    x = jnp.where(r == 0, a, jnp.where(r == 1, b, jnp.where(r == 2, c, 0.0)))
    return x.astype(BF16)


def sum3(y):
    return y[0:1] + y[1:2] + y[2:3]


def column(row):
    return jnp.concatenate(
        [
            jnp.broadcast_to(row[:, t : t + LANES], (LANES, LANES)).T
            for t in range(0, row.shape[1], LANES)
        ],
        0,
    )


def kernel(
    e_in, h_in, decay_in, gain_in, port_cell_in, port_node_in, port_cond_in, inv_in,
    line_near_in, line_far_in, line_delay_in, line_imped_in, hist_near_in, hist_far_in,
    e, h, volt_out, wave_out,
    port_cell, port_node, port_cond, line_near, line_far, line_delay, line_imped,
    hist_near, hist_far,
    e_top, decay, gain, gain_top, gain_send, gain_right, inv, inv2, pick, picked, own_pick,
    same, left, mat, cell_row, cell_y, row_right, y_right, node_hi, node_lo, pads,
    info_send, info, line_send, line_info, pre_send, pre, y_send, y, below, above,
    hz, ez_up, hx_send, hx, ex_send, ex, corner_send, corner_a, corner_b, acc,
    load_sem, face_ss, face_rs, info_ss, info_rs, pre_ss, pre_rs, y_ss, y_rs,
    up_ss, up_rs, down_ss, down_rs,
):
    s, j = lax.axis_index("fz"), lax.axis_index("fxy")
    ns, nj = lax.axis_size("fz"), lax.axis_size("fxy")
    above_id, below_id = lax.rem(s + 1, ns), lax.rem(s + ns - 1, ns)
    right_id, left_id = lax.rem(j + 1, nj), lax.rem(j + nj - 1, nj)
    has_above, has_below = s < ns - 1, s > 0
    has_right, has_left = j < nj - 1, j > 0
    _, cz, cx, ny = e_in.shape
    cells = cz * cx
    block, nodes = inv_in.shape[1:]
    ports = port_cell_in.shape[1]
    lines = line_near_in.shape[1]
    depth = hist_near_in.shape[0]
    pack = LANES // ports
    tiles = nj // pack
    np_ = nj * ports
    nt = np_ + 2 * lines

    loads = [
        pltpu.make_async_copy(e_in, e, load_sem.at[0]),
        pltpu.make_async_copy(gain_in, gain, load_sem.at[1]),
        pltpu.make_async_copy(h_in, h, load_sem.at[2]),
        pltpu.make_async_copy(decay_in, decay, load_sem.at[3]),
        pltpu.make_async_copy(inv_in.at[0], inv, load_sem.at[4]),
    ]
    small = (
        (port_cell_in, port_cell), (port_node_in, port_node), (port_cond_in, port_cond),
        (line_near_in, line_near), (line_far_in, line_far), (line_delay_in, line_delay),
        (line_imped_in, line_imped), (hist_near_in, hist_near), (hist_far_in, hist_far),
    )
    small = [
        pltpu.make_async_copy(src, dst, load_sem.at[5 + k])
        for k, (src, dst) in enumerate(small)
    ]
    for copy in small + loads[:4]:
        copy.start()

    e_top[...] = jnp.zeros(e_top.shape, F32)
    below[...] = jnp.zeros(below.shape, F32)
    above[...] = jnp.zeros(above.shape, F32)
    corner_a[...] = jnp.zeros(corner_a.shape, F32)
    corner_b[...] = jnp.zeros(corner_b.shape, F32)
    line_info[...] = (iota(line_info.shape, 0) == 2).astype(F32)

    barrier = pltpu.get_barrier_semaphore()
    for other in (above_id, below_id):
        pl.semaphore_signal(barrier, inc=1, device_id={"fz": other}, device_id_type=MESH)
    for d in range(1, nj):
        pl.semaphore_signal(
            barrier, inc=1, device_id={"fxy": lax.rem(j + d, nj)}, device_id_type=MESH
        )

    def remote(src, dst, ss, rs, **where):
        return pltpu.make_async_remote_copy(
            src_ref=src, dst_ref=dst, send_sem=ss, recv_sem=rs,
            device_id=where, device_id_type=MESH,
        )

    def face(kind, n, src, dst, **where):
        return remote(src, dst, face_ss.at[kind, n], face_rs.at[kind, n], **where)

    def when(cond, copies, act):
        @pl.when(cond)
        def _():
            for copy in copies:
                getattr(copy, act)()

    def up_z(n):
        return face(0, n, h.at[0:2, cz - 1], hz.at[n], fz=above_id)

    def up_x(n):
        return face(1, n, hx_send.at[n], hx.at[n], fxy=right_id)

    def down_z(n):
        return face(2, n, e.at[0:2, 0], ez_up.at[n], fz=below_id)

    def down_x(n):
        return face(3, n, ex_send.at[n], ex.at[n], fxy=left_id)

    def corner_down(n):
        return face(4, n, corner_send.at[n, 0], corner_a.at[n], fz=below_id, fxy=right_id)

    def corner_up(n):
        return face(5, n, corner_send.at[n, 1], corner_b.at[n], fz=above_id, fxy=left_id)

    line_copy = face(6, 0, line_send, line_info, fz=above_id)
    gain_z = face(6, 1, gain.at[0], gain_top, fz=below_id)
    gain_x = face(6, 2, gain_send, gain_right, fxy=left_id)

    def spread(src, dst, ss, rs):
        return [
            remote(src, dst, ss.at[d - 1], rs.at[d - 1], fxy=lax.rem(j + d, nj))
            for d in range(1, nj)
        ]

    def spread_z(src, dst, ss, rs, to):
        return [
            remote(src, dst, ss.at[d], rs.at[d], fz=to, fxy=lax.rem(j + d, nj))
            for d in range(nj)
        ]

    info_copies = spread(info_send, info.at[j], info_ss, info_rs)

    def pre_copies(n):
        return spread(pre_send.at[n], pre.at[n, j], pre_ss.at[n], pre_rs.at[n])

    def y_copies(n):
        return (
            spread(y_send.at[n], y.at[n, j], y_ss.at[n], y_rs.at[n]),
            spread_z(
                y_send.at[n, :, np_ : np_ + lines], below.at[n, j],
                up_ss.at[n], up_rs.at[n], above_id,
            ),
            spread_z(
                y_send.at[n, :, np_ + lines : nt], above.at[n, j],
                down_ss.at[n], down_rs.at[n], below_id,
            ),
        )

    def send_y(n, value):
        y_send[n] = value
        y[n, j] = value
        slab, up, down = y_copies(n)
        when(has_above, up, "start")
        when(has_below, down, "start")
        for copy in slab:
            copy.start()

    def pack_h(n):
        for c in range(2):
            for z in range(cz):
                hx_send[n, c, z : z + 1, :] = h[1 + c, z, cx - 1 : cx, :]
        corner_send[n, 0] = h[2, 0, cx - 1 : cx, :]
        corner_send[n, 1] = h[0, cz - 1, 0:1, :]

    def send_h(n):
        when(has_above, [up_z(n)], "start")
        when(has_right, [up_x(n)], "start")

    def send_corners(n):
        when(has_below & has_right, [corner_down(n)], "start")
        when(has_above & has_left, [corner_up(n)], "start")

    def send_e(n):
        for c in range(2):
            for z in range(cz):
                ex_send[n, c, z : z + 1, :] = e[1 + c, z, 0:1, :]
        when(has_below, [down_z(n)], "start")
        when(has_left, [down_x(n)], "start")

    lane = iota((cx, ny), 1)
    sub = iota((cx, ny), 0)

    def by(f):
        return f - jnp.where(lane == 0, 0.0, pltpu.roll(f, 1, 1))

    def bx(f):
        return f - jnp.where(sub == 0, 0.0, pltpu.roll(f, 1, 0))


    def update_ez():
        for z in range(cz):
            e[2, z] = decay[z] * e[2, z] + gain[z] * (bx(h[1, z]) - by(h[0, z]))

    def update_exy():
        for z in range(cz):
            dx, dy, hz_ = h[0, z], h[1, z], h[2, z]
            if z:
                dx, dy = dx - h[0, z - 1], dy - h[1, z - 1]
            e[0, z] = decay[z] * e[0, z] + gain[z] * (by(hz_) - dy)
            e[1, z] = decay[z] * e[1, z] + gain[z] * (dx - bx(hz_))

    def update_h():
        def plane(z, ux, uy):
            ex_, ey_, ez_ = (e[c, z] for c in range(3))

            def dy(f):
                return jnp.where(lane == ny - 1, 0.0, pltpu.roll(f, ny - 1, 1)) - f

            def dx(f):
                return jnp.where(sub == cx - 1, 0.0, pltpu.roll(f, cx - 1, 0)) - f

            h[0, z] = h[0, z] - 0.5 * (dy(ez_) - (uy - ey_))
            h[1, z] = h[1, z] - 0.5 * ((ux - ex_) - dx(ez_))
            h[2, z] = h[2, z] - 0.5 * (dx(ey_) - dy(ex_))

        @pl.loop(0, cz - 1, unroll=True)
        def _(z):
            plane(z, e[0, z + 1], e[1, z + 1])

        plane(cz - 1, e_top[0], e_top[1])

    for copy in small:
        copy.wait()

    pads[...] = jnp.zeros(pads.shape, F32)
    pads[0:1, 0:ports] = (port_cell[...] + 1).astype(F32)
    pads[1:2, 0:ports] = (port_node[...] + 1).astype(F32)
    pads[2:3, 0:ports] = port_cond[...]
    rows = pltpu.roll(pads[...], ports * lax.rem(j, pack), 1)
    info_send[...] = rows
    cell = rows[0:1].astype(I32) - 1
    valid = cell >= 0
    cell_row[...] = (
        iota((cells, LANES), 0) == jnp.where(valid, cell // ny, -1)
    ).astype(F32)
    cell_y[...] = (
        (iota((ny, LANES), 0) == jnp.where(valid, cell % ny, -1)).astype(F32).astype(BF16)
    )
    line_send[...] = jnp.zeros(line_send.shape, F32)
    line_send[0:1, :] = (line_far[...] + 1).astype(F32)
    line_send[1:2, :] = line_delay[...].astype(F32)
    line_send[2:3, :] = line_imped[...]
    for k in range(depth):
        line_send[3 + k : 4 + k, :] = hist_near[k]
        line_send[3 + depth + k : 4 + depth + k, :] = hist_far[k]

    def gather_cells(f):
        value = dot3(f.reshape(cells, ny), cell_y[...], ROWS)
        return jnp.sum(value * cell_row[...], axis=0, keepdims=True)

    loads[0].wait()
    loads[4].start()
    info_send[4:5, :] = gather_cells(e[2])
    loads[1].wait()
    info_send[3:4, :] = gather_cells(gain[...])
    for z in range(cz):
        gain_send[z : z + 1, :] = gain[z, 0:1, :]
    info[j] = info_send[...]

    pl.semaphore_wait(barrier, nj + 1)
    for copy in info_copies:
        copy.start()
    when(has_above, [line_copy], "start")
    when(has_below, [gain_z], "start")
    loads[2].wait()
    pack_h(0)
    send_h(0)
    when(has_left, [gain_x], "start")
    loads[3].wait()
    update_ez()
    update_exy()
    send_e(0)
    loads[4].wait()

    chunk = 32

    @pl.loop(0, block // chunk)
    def _(r):
        at = pl.ds(pl.multiple_of(r * chunk, chunk), chunk)
        x = inv[at, :]
        high = x.astype(BF16)
        inv2[at, :] = high
        inv2[pl.ds(pl.multiple_of(block + r * chunk, chunk), chunk), :] = (
            x - high.astype(F32)
        ).astype(BF16)

    wide = 2 * LANES

    def take_columns(first, last, index):
        @pl.loop(0, nodes // LANES)
        def _(r):
            at = pl.ds(pl.multiple_of(r * LANES, LANES), LANES)
            hit = iota((LANES, last - first), 0) + r * LANES == index
            pick[at, first:last] = hit.astype(F32).astype(BF16)

        for c in range(first, last, wide):
            at = slice(c, min(c + wide, last))
            for half in range(2):
                rows = slice(half * block, (half + 1) * block)
                picked[rows, at] = dot(inv2[rows, :], pick[:, at]).astype(BF16)

    when(has_above, [gain_z], "wait_recv")
    when(has_below, [line_copy], "wait_recv")
    send_corners(0)
    near_far = jnp.concatenate([line_near[...], line_info[0:1, :].astype(I32) - 1], 1)
    take_columns(np_, nt, near_far)
    for copy in info_copies:
        copy.wait_recv()

    everyone = jnp.concatenate(
        [sum(info[t * pack + k] for k in range(pack)) for t in range(tiles)], 1
    )
    cell_all = everyone[0:1] - 1.0
    cond_all, gain_all = everyone[2:3], everyone[3:4]
    index = jnp.concatenate([everyone[1:2].astype(I32) - 1, near_far], 1)
    high = jnp.where(index >= 0, index // block, -1)
    low = jnp.where(index >= 0, index % block, -1)
    node_hi[...] = (iota(node_hi.shape, 0) == high).astype(F32)
    node_lo[...] = (iota(node_lo.shape, 0) == low).astype(F32).astype(BF16)

    delay = jnp.concatenate([line_delay[...].astype(F32), line_info[1:2, :]], 0)
    scale = -2.0 / jnp.concatenate([line_imped[...], line_info[2:3, :]], 0)
    past_a = [
        jnp.concatenate([hist_near[k], line_info[3 + k : 4 + k, :]], 0)
        for k in range(depth)
    ]
    past_b = [
        jnp.concatenate([hist_far[k], line_info[3 + depth + k : 4 + depth + k, :]], 0)
        for k in range(depth)
    ]
    waves_a, waves_b = [], []

    def incoming(n, waves, past):
        total = jnp.zeros((2, lines), F32)
        for k in range(1, depth + 1):
            value = waves[n - k] if n >= k else past[k - n - 1]
            total = jnp.where(delay == k, value, total)
        return total

    def sources(n, ez):
        in_a, in_b = incoming(n, waves_b, past_b), incoming(n, waves_a, past_a)
        return in_a, in_b, jnp.concatenate([cond_all * ez, -in_a[0:1], -in_b[1:2]], 1)

    def own_volts(src):
        totals = dot3(node_hi[...] * src, node_lo[...], COLS)[0:nj]

        @pl.loop(0, block // chunk)
        def _(r):
            at = pl.ds(pl.multiple_of(r * chunk, chunk), chunk)
            value = jnp.zeros((chunk, LANES), F32)
            for k in range(nodes // LANES):
                q, w = divmod(k * LANES, block)
                value = value + inv[at, k * LANES : (k + 1) * LANES] * totals[
                    q : q + 1, w : w + LANES
                ]
            acc[at, :] = value

        terms = jnp.concatenate(parts3(acc[...]), 1).astype(BF16)
        return dot(jnp.ones((16, 3 * LANES), BF16), terms, COLS)[0:1]

    key = cell_all + ((iota((1, np_), 1) // ports) * (cells * ny)).astype(F32)
    key_col = column(key)
    for t in range(0, np_, LANES):
        at = slice(t, t + LANES)
        same[:, at] = (key_col == key[:, at]).astype(F32) * cond_all[:, at]

    ez = everyone[4:5]
    in_a, in_b, src = sources(0, ez)
    v0 = sum3(dot(fold3(own_volts(src)), node_lo[...]))
    v0 = jnp.where(high == j, v0, 0.0)
    drive = lax.dot_general(
        jnp.broadcast_to(v0[:, 0:np_], (8, np_)), same[...], COLS,
        precision=lax.Precision.HIGHEST, preferred_element_type=F32,
    )[0:1]
    send_y(0, jnp.concatenate([gain_all * drive, v0[:, np_:]], 1))

    neighbour = info[right_id]
    cell_r = neighbour[0:1].astype(I32) - 1
    gain_r = neighbour[3:4]
    valid_r = (cell_r >= 0) & (lax.rem(cell_r // ny, cx) == 0) & has_right
    row_right[...] = (
        iota((cz, LANES), 0) == jnp.where(valid_r, cell_r // (cx * ny), -1)
    ).astype(F32)
    y_right[...] = (
        (iota((ny, LANES), 0) == jnp.where(valid_r, cell_r % ny, -1))
        .astype(F32)
        .astype(BF16)
    )

    def send_pre(n):
        value = gather_cells(e[2])
        side = dot3(hx_send[n - 1, 0], y_right[...], ROWS) * row_right[...]
        side = -gain_r * jnp.sum(side, axis=0, keepdims=True)
        for t in range(tiles):
            at = slice(t * LANES, (t + 1) * LANES)
            both = jnp.where(j // pack == t, value, 0.0)
            both = both + jnp.where(right_id // pack == t, side, 0.0)
            pre_send[n, :, at] = both
        pre[n, j] = pre_send[n]
        for copy in pre_copies(n):
            copy.start()

    send_pre(1)

    cond_col = column(cond_all)
    gain_col = column(gain_all)
    load, first = [], []
    for t in range(0, np_, LANES):
        hit = key_col == key[:, t : t + LANES]
        load.append(jnp.sum(jnp.where(hit, cond_col, 0.0), axis=0, keepdims=True))
        earlier = hit & (iota(hit.shape, 0) < iota(hit.shape, 1) + t)
        first.append(jnp.max(earlier.astype(F32), axis=0, keepdims=True))
    load = gain_all * jnp.concatenate(load, 1)
    first = 1.0 - jnp.concatenate(first, 1)

    take_columns(0, np_, index[:, 0:np_])
    index_col = column(index.astype(F32))
    for w in range(0, block, LANES):
        node = (iota((nt, LANES), 1) + (w + j * block)).astype(F32)
        own_pick[:, w : w + LANES] = (index_col == node).astype(F32).astype(BF16)
    mixed = dot3(same[...], own_pick[0:np_, :], ROWS)
    for w in range(0, block, LANES):
        at = slice(w, w + LANES)
        value = mixed[:, at] * gain_col
        high_ = value.astype(BF16)
        left[0:np_, at] = high_
        left[np_ : 2 * np_, at] = (value - high_.astype(F32)).astype(BF16)
    left[2 * np_ :, :] = own_pick[np_:, :]
    upper = dot(left[...], picked[0:block, :])
    lower = dot(left[0:np_, :], picked[block:, :])
    value = upper[0:np_] + (upper[np_ : 2 * np_] + lower)
    high_ = value.astype(BF16)
    mat[0:np_, 0:nt] = high_
    mat[0:np_, nt:] = (value - high_.astype(F32)).astype(BF16)
    mat[np_:, 0:nt] = upper[2 * np_ :].astype(BF16)
    mat[np_:, nt:] = dot(left[2 * np_ :, :], picked[block:, :]).astype(BF16)

    def tile_of(x, device):
        out = x[:, 0:LANES]
        for t in range(1, tiles):
            out = jnp.where(device // pack == t, x[:, t * LANES : (t + 1) * LANES], out)
        return out

    when(has_right, [gain_x], "wait_recv")
    at_x = slice(cx - 1, cx)

    for n in range(STEPS):
        slab, up, down = y_copies(n)
        for copy in slab:
            copy.wait_recv()
        when(has_below, up, "wait_recv")
        when(has_above, down, "wait_recv")
        total, v_below, v_above = y[n, 0], below[n, 0], above[n, 0]
        for k in range(1, nj):
            total = total + y[n, k]
            v_below = v_below + below[n, k]
            v_above = v_above + above[n, k]
        v_near = jnp.concatenate([total[:, np_ : np_ + lines], v_below], 0)
        v_far = jnp.concatenate([v_above, total[:, np_ + lines :]], 0)
        waves_a.append(scale * v_near - in_a)
        waves_b.append(scale * v_far - in_b)
        change = total[:, 0:np_] - load * ez
        once = change * first
        drop = dot3(cell_row[...] * tile_of(once, j), cell_y[...], COLS)

        when(has_below, [down_z(n)], "wait_send")

        @pl.when(has_left)
        def _():
            up_x(n).wait_recv()
            for z in range(cz):
                g = gain[z, 0:1, :]
                e[1, z, 0:1, :] = e[1, z, 0:1, :] + g * hx[n, 1, z : z + 1, :]
                e[2, z, 0:1, :] = e[2, z, 0:1, :] - g * hx[n, 0, z : z + 1, :]

        @pl.when(has_below)
        def _():
            up_z(n).wait_recv()
            g = gain[0]
            e[0, 0] = e[0, 0] + g * hz[n, 1]
            e[1, 0] = e[1, 0] - g * hz[n, 0]

        e[2] = e[2] + drop.reshape(cz, cx, ny)
        if n + 1 < STEPS:
            for copy in pre_copies(n + 1):
                copy.wait_recv()
            ez = change + pre[n + 1, 0]
            for k in range(1, nj):
                ez = ez + pre[n + 1, k]
            in_a, in_b, src = sources(n + 1, ez)
            x = fold3(src)
            send_y(n + 1, sum3(dot(jnp.concatenate([x, x], 1), mat[...], COLS)))
        when(has_above & has_left, [corner_down(n)], "wait_recv")
        when(has_below & has_right, [corner_up(n)], "wait_recv")

        @pl.when(has_above)
        def _():
            down_z(n).wait_recv()
            e_top[0] = ez_up[n, 0] + gain_top[...] * h[1, cz - 1]
            e_top[1] = ez_up[n, 1] - gain_top[...] * h[0, cz - 1]
            e_top[1, 0:1, :] = e_top[1, 0:1, :] + gain_top[0:1, :] * corner_a[n]
            up_z(n).wait_send()

        drop_right = dot3(row_right[...] * tile_of(once, right_id), y_right[...], COLS)
        update_h()

        @pl.when(has_right)
        def _():
            down_x(n).wait_recv()
            g = gain_right[...]
            face_y = ex[n, 0] + g * hx_send[n, 1]
            face_z = ex[n, 1] - g * hx_send[n, 0] + drop_right
            for z in range(cz):
                y_ = face_y[z : z + 1]
                if z == 0:
                    y_ = y_ - g[0:1] * corner_b[n]
                h[1, z, at_x, :] = h[1, z, at_x, :] + 0.5 * face_z[z : z + 1]
                h[2, z, at_x, :] = h[2, z, at_x, :] - 0.5 * y_

        if n + 1 < STEPS:
            pack_h(n + 1)
            update_ez()
            if n + 2 < STEPS:
                send_pre(n + 2)
            send_h(n + 1)
            send_corners(n + 1)
            update_exy()
            send_e(n + 1)
        if n + 2 == STEPS:
            volt_out[...] = own_volts(src)

    wave_out[0, 0:1, :] = waves_a[-1][0:1]
    wave_out[0, 1:2, :] = waves_b[-1][0:1]

    for copy in info_copies:
        copy.wait_send()
    when(has_above, [line_copy], "wait_send")
    when(has_below, [gain_z], "wait_send")
    when(has_left, [gain_x], "wait_send")
    for n in range(STEPS):
        slab, up, down = y_copies(n)
        for copy in slab:
            copy.wait_send()
        when(has_above, up, "wait_send")
        when(has_below, down, "wait_send")
        if n:
            for copy in pre_copies(n):
                copy.wait_send()
        when(has_right, [up_x(n)], "wait_send")
        when(has_left, [down_x(n)], "wait_send")
        when(has_below & has_right, [corner_down(n)], "wait_send")
        when(has_above & has_left, [corner_up(n)], "wait_send")


def local(*args):
    e_field, inverse = args[0], args[7]
    nj = lax.axis_size("fxy")
    _, cz, cx, ny = e_field.shape
    _, block, nodes = inverse.shape
    ports, lines = args[4].shape[1], args[8].shape[1]
    args = [*args[:12], *(a.transpose(1, 0, 2) for a in args[12:])]
    depth = args[12].shape[0]
    vmem = pl.BlockSpec(memory_space=pltpu.VMEM)
    hbm = pl.BlockSpec(memory_space=pltpu.HBM)
    small = [a for i, a in enumerate(args) if i not in (0, 1, 2, 3, 7)]
    rows = -(-nj // 16) * 16
    np_ = nj * ports
    nt = np_ + 2 * lines
    line_rows = -(-(3 + 2 * depth) // 8) * 8
    dma = pltpu.SemaphoreType.DMA
    v = pltpu.VMEM
    e, h, volt, wave = pl.pallas_call(
        kernel,
        out_shape=(
            v(e_field.shape, F32),
            v(e_field.shape, F32),
            v((1, block), F32),
            v((1, 2, lines), F32),
        ),
        in_specs=[hbm] * len(args),
        out_specs=(vmem,) * 4,
        scratch_shapes=[
            *[v(a.shape, a.dtype) for a in small],
            v((2, cx, ny), F32),
            v((cz, cx, ny), F32),
            v((cz, cx, ny), F32),
            v((cx, ny), F32),
            v((cz, ny), F32),
            v((cz, ny), F32),
            v((block, nodes), F32),
            v((2 * block, nodes), BF16),
            v((nodes, nt), BF16),
            v((2 * block, nt), BF16),
            v((nt, block), BF16),
            v((np_, np_), F32),
            v((2 * np_ + 2 * lines, block), BF16),
            v((nt, 2 * nt), BF16),
            v((cz * cx, LANES), F32),
            v((ny, LANES), BF16),
            v((cz, LANES), F32),
            v((ny, LANES), BF16),
            v((rows, nt), F32),
            v((block, nt), BF16),
            v((8, LANES), F32),
            v((8, LANES), F32),
            v((nj, 8, LANES), F32),
            v((line_rows, lines), F32),
            v((line_rows, lines), F32),
            v((STEPS, 1, np_), F32),
            v((STEPS, nj, 1, np_), F32),
            v((STEPS, 1, nt), F32),
            v((STEPS, nj, 1, nt), F32),
            v((STEPS, nj, 1, lines), F32),
            v((STEPS, nj, 1, lines), F32),
            v((STEPS, 2, cx, ny), F32),
            v((STEPS, 2, cx, ny), F32),
            v((STEPS, 2, cz, ny), F32),
            v((STEPS, 2, cz, ny), F32),
            v((STEPS, 2, cz, ny), F32),
            v((STEPS, 2, cz, ny), F32),
            v((STEPS, 2, 1, ny), F32),
            v((STEPS, 1, ny), F32),
            v((STEPS, 1, ny), F32),
            v((block, LANES), F32),
            dma((5 + len(small),)),
            dma((7, STEPS)),
            dma((7, STEPS)),
            dma((nj - 1,)),
            dma((nj - 1,)),
            dma((STEPS, nj - 1)),
            dma((STEPS, nj - 1)),
            dma((STEPS, nj - 1)),
            dma((STEPS, nj - 1)),
            dma((STEPS, nj)),
            dma((STEPS, nj)),
            dma((STEPS, nj)),
            dma((STEPS, nj)),
        ],
        compiler_params=pltpu.CompilerParams(
            collective_id=0, has_side_effects=True, vmem_limit_bytes=61 * 1024 * 1024
        ),
    )(*args)
    outs = [pltpu.with_memory_space_constraint(x, pltpu.VMEM) for x in (e, h, volt, wave)]
    return pl.pallas_call(
        store,
        out_shape=[jax.ShapeDtypeStruct(x.shape, F32) for x in outs],
        in_specs=[vmem] * 4,
        out_specs=[hbm] * 4,
        scratch_shapes=[dma((4,))],
    )(*outs)


def store(e, h, volt, wave, e_out, h_out, volt_out, wave_out, sem):
    pairs = ((e, e_out), (h, h_out), (volt, volt_out), (wave, wave_out))
    copies = [pltpu.make_async_copy(a, b, sem.at[k]) for k, (a, b) in enumerate(pairs)]
    for copy in copies:
        copy.start()
    for copy in copies:
        copy.wait()


def solution(mesh):
    placed = (
        P(None, "fz", "fxy", None),
        P(None, "fz", "fxy", None),
        P("fz", "fxy", None),
        P("fz", "fxy", None),
        P("fz", "fxy"),
        P("fz", "fxy"),
        P("fz", "fxy"),
        P("fz", "fxy", None),
        P("fz", None),
        P("fz", None),
        P("fz", None),
        P("fz", None),
        P("fz", None, None),
        P("fz", None, None),
    )
    return jax.shard_map(
        local,
        mesh=mesh,
        in_specs=placed,
        out_specs=(
            P(None, "fz", "fxy", None),
            P(None, "fz", "fxy", None),
            P("fz", "fxy"),
            P("fz", None, None),
        ),
        check_vma=False,
    )
```

```python
import jax
import jax.numpy as jnp
from jax import lax
from jax.experimental import pallas as pl
from jax.experimental.pallas import tpu as pltpu
from jax.sharding import PartitionSpec as P

STEPS = 4
LANES = 128
F32 = jnp.float32
BF16 = jnp.bfloat16
I32 = jnp.int32
MESH = pl.DeviceIdType.MESH
ROWS = (((1,), (0,)), ((), ()))
COLS = (((1,), (1,)), ((), ()))


def iota(shape, dim):
    return lax.broadcasted_iota(I32, shape, dim)


def parts3(x):
    a = x.astype(BF16).astype(F32)
    r = x - a
    b = r.astype(BF16).astype(F32)
    return a, b, r - b


def dot(x, y, dims=ROWS):
    return lax.dot_general(x, y, dims, preferred_element_type=F32)


def dot3(x, onehot, dims):
    rows = x.shape[0]
    parts = list(parts3(x))
    pad = -3 * rows % 16
    if pad:
        parts.append(jnp.zeros((pad, x.shape[1]), F32))
    y = dot(jnp.concatenate(parts, 0).astype(BF16), onehot, dims)
    return y[:rows] + y[rows : 2 * rows] + y[2 * rows : 3 * rows]


def fold3(x):
    a, b, c = parts3(jnp.broadcast_to(x, (16, x.shape[1])))
    r = iota(a.shape, 0)
    x = jnp.where(r == 0, a, jnp.where(r == 1, b, jnp.where(r == 2, c, 0.0)))
    return x.astype(BF16)


def sum3(y):
    return y[0:1] + y[1:2] + y[2:3]


def column(row):
    return jnp.concatenate(
        [
            jnp.broadcast_to(row[:, t : t + LANES], (LANES, LANES)).T
            for t in range(0, row.shape[1], LANES)
        ],
        0,
    )


def kernel(
    e_in, h_in, decay_in, gain_in, port_cell_in, port_node_in, port_cond_in, inv_in,
    line_near_in, line_far_in, line_delay_in, line_imped_in, hist_near_in, hist_far_in,
    e, h, volt_out, wave_out,
    port_cell, port_node, port_cond, line_near, line_far, line_delay, line_imped,
    hist_near, hist_far,
    decay, gain, gain_top, gain_send, gain_right, inv, inv2, pick, picked, own_pick,
    same, left, mat, cell_row, cell_y, row_right, y_right, node_hi, node_lo, pads,
    info_send, info, line_send, line_info, pre_send, pre, y_send, y, below, above,
    hz, ez_up, hx_send, hx, ex_send, ex, corner_send, corner_a, corner_b, acc,
    load_sem, face_ss, face_rs, info_ss, info_rs, pre_ss, pre_rs, y_ss, y_rs,
    up_ss, up_rs, down_ss, down_rs,
):
    s, j = lax.axis_index("fz"), lax.axis_index("fxy")
    ns, nj = lax.axis_size("fz"), lax.axis_size("fxy")
    above_id, below_id = lax.rem(s + 1, ns), lax.rem(s + ns - 1, ns)
    right_id, left_id = lax.rem(j + 1, nj), lax.rem(j + nj - 1, nj)
    has_above, has_below = s < ns - 1, s > 0
    has_right, has_left = j < nj - 1, j > 0
    _, cz, cx, ny = e_in.shape
    cells = cz * cx
    block, nodes = inv_in.shape[1:]
    ports = port_cell_in.shape[1]
    lines = line_near_in.shape[1]
    depth = hist_near_in.shape[0]
    pack = LANES // ports
    tiles = nj // pack
    np_ = nj * ports
    nt = np_ + 2 * lines

    loads = [
        pltpu.make_async_copy(e_in, e, load_sem.at[0]),
        pltpu.make_async_copy(gain_in, gain, load_sem.at[1]),
        pltpu.make_async_copy(h_in, h, load_sem.at[2]),
        pltpu.make_async_copy(decay_in, decay, load_sem.at[3]),
        pltpu.make_async_copy(inv_in.at[0], inv, load_sem.at[4]),
    ]
    small = (
        (port_cell_in, port_cell), (port_node_in, port_node), (port_cond_in, port_cond),
        (line_near_in, line_near), (line_far_in, line_far), (line_delay_in, line_delay),
        (line_imped_in, line_imped), (hist_near_in, hist_near), (hist_far_in, hist_far),
    )
    small = [
        pltpu.make_async_copy(src, dst, load_sem.at[5 + k])
        for k, (src, dst) in enumerate(small)
    ]
    for copy in small + loads[:4]:
        copy.start()

    below[...] = jnp.zeros(below.shape, F32)
    above[...] = jnp.zeros(above.shape, F32)
    corner_a[...] = jnp.zeros(corner_a.shape, F32)
    corner_b[...] = jnp.zeros(corner_b.shape, F32)
    line_info[...] = (iota(line_info.shape, 0) == 2).astype(F32)

    barrier = pltpu.get_barrier_semaphore()
    for other in (above_id, below_id):
        pl.semaphore_signal(barrier, inc=1, device_id={"fz": other}, device_id_type=MESH)
    for d in range(1, nj):
        pl.semaphore_signal(
            barrier, inc=1, device_id={"fxy": lax.rem(j + d, nj)}, device_id_type=MESH
        )

    for missing, refs in (
        (jnp.logical_not(has_below), (hz,)),
        (jnp.logical_not(has_above), (ez_up, gain_top)),
        (jnp.logical_not(has_left), (hx,)),
        (jnp.logical_not(has_right), (ex, gain_right)),
    ):

        @pl.when(missing)
        def _(refs=refs):
            for ref in refs:
                ref[...] = jnp.zeros(ref.shape, F32)

    def remote(src, dst, ss, rs, **where):
        return pltpu.make_async_remote_copy(
            src_ref=src, dst_ref=dst, send_sem=ss, recv_sem=rs,
            device_id=where, device_id_type=MESH,
        )

    def face(kind, n, src, dst, **where):
        return remote(src, dst, face_ss.at[kind, n], face_rs.at[kind, n], **where)

    def when(cond, copies, act):
        @pl.when(cond)
        def _():
            for copy in copies:
                getattr(copy, act)()

    def up_z(n):
        return face(0, n, h.at[0:2, cz - 1], hz.at[n], fz=above_id)

    def up_x(n):
        return face(1, n, hx_send.at[n], hx.at[n], fxy=right_id)

    def down_z(n):
        return face(2, n, e.at[0:2, 0], ez_up.at[n], fz=below_id)

    def down_x(n):
        return face(3, n, ex_send.at[n], ex.at[n], fxy=left_id)

    def corner_down(n):
        return face(4, n, corner_send.at[n, 0], corner_a.at[n], fz=below_id, fxy=right_id)

    def corner_up(n):
        return face(5, n, corner_send.at[n, 1], corner_b.at[n], fz=above_id, fxy=left_id)

    line_copy = face(6, 0, line_send, line_info, fz=above_id)
    gain_z = face(6, 1, gain.at[0], gain_top, fz=below_id)
    gain_x = face(6, 2, gain_send, gain_right, fxy=left_id)

    def spread(src, dst, ss, rs):
        return [
            remote(src, dst, ss.at[d - 1], rs.at[d - 1], fxy=lax.rem(j + d, nj))
            for d in range(1, nj)
        ]

    def spread_z(src, dst, ss, rs, to):
        return [
            remote(src, dst, ss.at[d], rs.at[d], fz=to, fxy=lax.rem(j + d, nj))
            for d in range(nj)
        ]

    info_copies = spread(info_send, info.at[j], info_ss, info_rs)

    def pre_copies(n):
        return spread(pre_send.at[n], pre.at[n, j], pre_ss.at[n], pre_rs.at[n])

    def y_copies(n):
        return (
            spread(y_send.at[n], y.at[n, j], y_ss.at[n], y_rs.at[n]),
            spread_z(
                y_send.at[n, :, np_ : np_ + lines], below.at[n, j],
                up_ss.at[n], up_rs.at[n], above_id,
            ),
            spread_z(
                y_send.at[n, :, np_ + lines : nt], above.at[n, j],
                down_ss.at[n], down_rs.at[n], below_id,
            ),
        )

    def send_y(n, value):
        y_send[n] = value
        y[n, j] = value
        slab, up, down = y_copies(n)
        when(has_above, up, "start")
        when(has_below, down, "start")
        for copy in slab:
            copy.start()

    def pack_h(n):
        for c in range(2):
            for z in range(cz):
                hx_send[n, c, z : z + 1, :] = h[1 + c, z, cx - 1 : cx, :]
        corner_send[n, 0] = h[2, 0, cx - 1 : cx, :]
        corner_send[n, 1] = h[0, cz - 1, 0:1, :]

    def send_h(n):
        when(has_above, [up_z(n)], "start")
        when(has_right, [up_x(n)], "start")

    def send_corners(n):
        when(has_below & has_right, [corner_down(n)], "start")
        when(has_above & has_left, [corner_up(n)], "start")

    def send_e(n):
        for c in range(2):
            for z in range(cz):
                ex_send[n, c, z : z + 1, :] = e[1 + c, z, 0:1, :]
        when(has_below, [down_z(n)], "start")
        when(has_left, [down_x(n)], "start")

    lane = iota((cx, ny), 1)
    sub = iota((cx, ny), 0)

    def by(f):
        return f - jnp.where(lane == 0, 0.0, pltpu.roll(f, 1, 1))

    def bx(f):
        return f - jnp.where(sub == 0, 0.0, pltpu.roll(f, 1, 0))


    def update_ez():
        for z in range(cz):
            e[2, z] = decay[z] * e[2, z] + gain[z] * (bx(h[1, z]) - by(h[0, z]))

    def update_exy():
        for z in range(cz):
            dx, dy, hz_ = h[0, z], h[1, z], h[2, z]
            if z:
                dx, dy = dx - h[0, z - 1], dy - h[1, z - 1]
            e[0, z] = decay[z] * e[0, z] + gain[z] * (by(hz_) - dy)
            e[1, z] = decay[z] * e[1, z] + gain[z] * (dx - bx(hz_))

    def update_h(top):
        def plane(z, ux, uy):
            ex_, ey_, ez_ = (e[c, z] for c in range(3))

            def dy(f):
                return jnp.where(lane == ny - 1, 0.0, pltpu.roll(f, ny - 1, 1)) - f

            def dx(f):
                return jnp.where(sub == cx - 1, 0.0, pltpu.roll(f, cx - 1, 0)) - f

            h[0, z] = h[0, z] - 0.5 * (dy(ez_) - (uy - ey_))
            h[1, z] = h[1, z] - 0.5 * ((ux - ex_) - dx(ez_))
            h[2, z] = h[2, z] - 0.5 * (dx(ey_) - dy(ex_))

        @pl.loop(0, cz - 1, unroll=True)
        def _(z):
            plane(z, e[0, z + 1], e[1, z + 1])

        plane(cz - 1, *top)

    for copy in small:
        copy.wait()

    pads[...] = jnp.zeros(pads.shape, F32)
    pads[0:1, 0:ports] = (port_cell[...] + 1).astype(F32)
    pads[1:2, 0:ports] = (port_node[...] + 1).astype(F32)
    pads[2:3, 0:ports] = port_cond[...]
    rows = pltpu.roll(pads[...], ports * lax.rem(j, pack), 1)
    info_send[...] = rows
    cell = rows[0:1].astype(I32) - 1
    valid = cell >= 0
    cell_row[...] = (
        iota((cells, LANES), 0) == jnp.where(valid, cell // ny, -1)
    ).astype(F32)
    cell_y[...] = (
        (iota((ny, LANES), 0) == jnp.where(valid, cell % ny, -1)).astype(F32).astype(BF16)
    )
    line_send[...] = jnp.zeros(line_send.shape, F32)
    line_send[0:1, :] = (line_far[...] + 1).astype(F32)
    line_send[1:2, :] = line_delay[...].astype(F32)
    line_send[2:3, :] = line_imped[...]
    for k in range(depth):
        line_send[3 + k : 4 + k, :] = hist_near[k]
        line_send[3 + depth + k : 4 + depth + k, :] = hist_far[k]

    def gather_cells(f):
        value = dot3(f.reshape(cells, ny), cell_y[...], ROWS)
        return jnp.sum(value * cell_row[...], axis=0, keepdims=True)

    loads[0].wait()
    loads[4].start()
    info_send[4:5, :] = gather_cells(e[2])
    loads[1].wait()
    info_send[3:4, :] = gather_cells(gain[...])
    for z in range(cz):
        gain_send[z : z + 1, :] = gain[z, 0:1, :]
    info[j] = info_send[...]

    pl.semaphore_wait(barrier, nj + 1)
    for copy in info_copies:
        copy.start()
    when(has_above, [line_copy], "start")
    when(has_below, [gain_z], "start")
    loads[2].wait()
    pack_h(0)
    send_h(0)
    when(has_left, [gain_x], "start")
    loads[3].wait()
    update_ez()
    update_exy()
    send_e(0)
    loads[4].wait()

    chunk = 32

    @pl.loop(0, block // chunk)
    def _(r):
        at = pl.ds(pl.multiple_of(r * chunk, chunk), chunk)
        x = inv[at, :]
        high = x.astype(BF16)
        inv2[at, :] = high
        inv2[pl.ds(pl.multiple_of(block + r * chunk, chunk), chunk), :] = (
            x - high.astype(F32)
        ).astype(BF16)

    wide = 2 * LANES

    def take_columns(first, last, index):
        @pl.loop(0, nodes // LANES)
        def _(r):
            at = pl.ds(pl.multiple_of(r * LANES, LANES), LANES)
            hit = iota((LANES, last - first), 0) + r * LANES == index
            pick[at, first:last] = hit.astype(F32).astype(BF16)

        for c in range(first, last, wide):
            at = slice(c, min(c + wide, last))
            for half in range(2):
                rows = slice(half * block, (half + 1) * block)
                picked[rows, at] = dot(inv2[rows, :], pick[:, at]).astype(BF16)

    when(has_above, [gain_z], "wait_recv")
    when(has_below, [line_copy], "wait_recv")
    send_corners(0)
    near_far = jnp.concatenate([line_near[...], line_info[0:1, :].astype(I32) - 1], 1)
    for copy in info_copies:
        copy.wait_recv()

    everyone = jnp.concatenate(
        [sum(info[t * pack + k] for k in range(pack)) for t in range(tiles)], 1
    )
    cell_all = everyone[0:1] - 1.0
    cond_all, gain_all = everyone[2:3], everyone[3:4]
    index = jnp.concatenate([everyone[1:2].astype(I32) - 1, near_far], 1)
    high = jnp.where(index >= 0, index // block, -1)
    low = jnp.where(index >= 0, index % block, -1)
    node_hi[...] = (iota(node_hi.shape, 0) == high).astype(F32)
    node_lo[...] = (iota(node_lo.shape, 0) == low).astype(F32).astype(BF16)

    delay = jnp.concatenate([line_delay[...].astype(F32), line_info[1:2, :]], 0)
    scale = -2.0 / jnp.concatenate([line_imped[...], line_info[2:3, :]], 0)
    past_a = [
        jnp.concatenate([hist_near[k], line_info[3 + k : 4 + k, :]], 0)
        for k in range(depth)
    ]
    past_b = [
        jnp.concatenate([hist_far[k], line_info[3 + depth + k : 4 + depth + k, :]], 0)
        for k in range(depth)
    ]
    waves_a, waves_b = [], []

    def incoming(n, waves, past):
        total = jnp.zeros((2, lines), F32)
        for k in range(1, depth + 1):
            value = waves[n - k] if n >= k else past[k - n - 1]
            total = jnp.where(delay == k, value, total)
        return total

    def sources(n, ez):
        in_a, in_b = incoming(n, waves_b, past_b), incoming(n, waves_a, past_a)
        return in_a, in_b, jnp.concatenate([cond_all * ez, -in_a[0:1], -in_b[1:2]], 1)

    def own_volts(src):
        totals = dot3(node_hi[...] * src, node_lo[...], COLS)[0:nj]

        @pl.loop(0, block // chunk, unroll=4)
        def _(r):
            at = pl.ds(pl.multiple_of(r * chunk, chunk), chunk)
            value = jnp.zeros((chunk, LANES), F32)
            for k in range(nodes // LANES):
                q, w = divmod(k * LANES, block)
                value = value + inv[at, k * LANES : (k + 1) * LANES] * totals[
                    q : q + 1, w : w + LANES
                ]
            acc[at, :] = value

        terms = jnp.concatenate(parts3(acc[...]), 1).astype(BF16)
        return dot(jnp.ones((16, 3 * LANES), BF16), terms, COLS)[0:1]

    key = cell_all + ((iota((1, np_), 1) // ports) * (cells * ny)).astype(F32)
    key_col = column(key)
    for t in range(0, np_, LANES):
        at = slice(t, t + LANES)
        same[:, at] = (key_col == key[:, at]).astype(F32) * cond_all[:, at]

    ez = everyone[4:5]
    in_a, in_b, src = sources(0, ez)
    v0 = sum3(dot(fold3(own_volts(src)), node_lo[...]))
    v0 = jnp.where(high == j, v0, 0.0)
    drive = lax.dot_general(
        jnp.broadcast_to(v0[:, 0:np_], (8, np_)), same[...], COLS,
        precision=lax.Precision.HIGHEST, preferred_element_type=F32,
    )[0:1]
    send_y(0, jnp.concatenate([gain_all * drive, v0[:, np_:]], 1))

    neighbour = info[right_id]
    cell_r = neighbour[0:1].astype(I32) - 1
    gain_r = neighbour[3:4]
    valid_r = (cell_r >= 0) & (lax.rem(cell_r // ny, cx) == 0) & has_right
    row_right[...] = (
        iota((cz, LANES), 0) == jnp.where(valid_r, cell_r // (cx * ny), -1)
    ).astype(F32)
    y_right[...] = (
        (iota((ny, LANES), 0) == jnp.where(valid_r, cell_r % ny, -1))
        .astype(F32)
        .astype(BF16)
    )

    def send_pre(n):
        value = gather_cells(e[2])
        side = dot3(hx_send[n - 1, 0], y_right[...], ROWS) * row_right[...]
        side = -gain_r * jnp.sum(side, axis=0, keepdims=True)
        for t in range(tiles):
            at = slice(t * LANES, (t + 1) * LANES)
            both = jnp.where(j // pack == t, value, 0.0)
            both = both + jnp.where(right_id // pack == t, side, 0.0)
            pre_send[n, :, at] = both
        pre[n, j] = pre_send[n]
        for copy in pre_copies(n):
            copy.start()

    send_pre(1)

    cond_col = column(cond_all)
    gain_col = column(gain_all)
    load, first = [], []
    for t in range(0, np_, LANES):
        hit = key_col == key[:, t : t + LANES]
        load.append(jnp.sum(jnp.where(hit, cond_col, 0.0), axis=0, keepdims=True))
        earlier = hit & (iota(hit.shape, 0) < iota(hit.shape, 1) + t)
        first.append(jnp.max(earlier.astype(F32), axis=0, keepdims=True))
    load = gain_all * jnp.concatenate(load, 1)
    first = 1.0 - jnp.concatenate(first, 1)

    take_columns(0, np_, index[:, 0:np_])
    take_columns(np_, nt, index[:, np_:nt])
    index_col = column(index.astype(F32))
    for w in range(0, block, LANES):
        node = (iota((nt, LANES), 1) + (w + j * block)).astype(F32)
        own_pick[:, w : w + LANES] = (index_col == node).astype(F32).astype(BF16)
    mixed = dot3(same[...], own_pick[0:np_, :], ROWS)
    for w in range(0, block, LANES):
        at = slice(w, w + LANES)
        value = mixed[:, at] * gain_col
        high_ = value.astype(BF16)
        left[0:np_, at] = high_
        left[np_ : 2 * np_, at] = (value - high_.astype(F32)).astype(BF16)
    left[2 * np_ :, :] = own_pick[np_:, :]
    upper = dot(left[...], picked[0:block, :])
    lower = dot(left[0:np_, :], picked[block:, :])
    value = upper[0:np_] + (upper[np_ : 2 * np_] + lower)
    high_ = value.astype(BF16)
    mat[0:np_, 0:nt] = high_
    mat[0:np_, nt:] = (value - high_.astype(F32)).astype(BF16)
    mat[np_:, 0:nt] = upper[2 * np_ :].astype(BF16)
    mat[np_:, nt:] = dot(left[2 * np_ :, :], picked[block:, :]).astype(BF16)

    def tile_of(x, device):
        out = x[:, 0:LANES]
        for t in range(1, tiles):
            out = jnp.where(device // pack == t, x[:, t * LANES : (t + 1) * LANES], out)
        return out

    when(has_right, [gain_x], "wait_recv")
    at_x = slice(cx - 1, cx)

    for n in range(STEPS):
        slab, up, down = y_copies(n)
        for copy in slab:
            copy.wait_recv()
        when(has_below, up, "wait_recv")
        when(has_above, down, "wait_recv")
        total, v_below, v_above = y[n, 0], below[n, 0], above[n, 0]
        for k in range(1, nj):
            total = total + y[n, k]
            v_below = v_below + below[n, k]
            v_above = v_above + above[n, k]
        v_near = jnp.concatenate([total[:, np_ : np_ + lines], v_below], 0)
        v_far = jnp.concatenate([v_above, total[:, np_ + lines :]], 0)
        waves_a.append(scale * v_near - in_a)
        waves_b.append(scale * v_far - in_b)
        change = total[:, 0:np_] - load * ez
        once = change * first
        drop = dot3(cell_row[...] * tile_of(once, j), cell_y[...], COLS)

        if n + 1 < STEPS:
            for copy in pre_copies(n + 1):
                copy.wait_recv()
            ez = change + pre[n + 1, 0]
            for k in range(1, nj):
                ez = ez + pre[n + 1, k]
            in_a, in_b, src = sources(n + 1, ez)
            x = fold3(src)
            send_y(n + 1, sum3(dot(jnp.concatenate([x, x], 1), mat[...], COLS)))
        when(has_below, [down_z(n)], "wait_send")
        when(has_above, [up_z(n)], "wait_send")
        when(has_left, [up_x(n)], "wait_recv")
        when(has_below, [up_z(n)], "wait_recv")
        when(has_above, [down_z(n)], "wait_recv")
        when(has_right, [down_x(n)], "wait_recv")
        when(has_above & has_left, [corner_down(n)], "wait_recv")
        when(has_below & has_right, [corner_up(n)], "wait_recv")
        for z in range(cz):
            g = gain[z, 0:1, :]
            e[1, z, 0:1, :] = e[1, z, 0:1, :] + g * hx[n, 1, z : z + 1, :]
            e[2, z, 0:1, :] = e[2, z, 0:1, :] - g * hx[n, 0, z : z + 1, :]
        e[0, 0] = e[0, 0] + gain[0] * hz[n, 1]
        e[1, 0] = e[1, 0] - gain[0] * hz[n, 0]
        e[2] = e[2] + drop.reshape(cz, cx, ny)
        top_x = ez_up[n, 0] + gain_top[...] * h[1, cz - 1]
        side = jnp.where(sub == 0, gain_top[0:1, :] * corner_a[n], 0.0)
        top_y = ez_up[n, 1] - gain_top[...] * h[0, cz - 1] + side
        drop_right = dot3(row_right[...] * tile_of(once, right_id), y_right[...], COLS)
        g = gain_right[...]
        face_y = ex[n, 0] + g * hx_send[n, 1]
        face_z = ex[n, 1] - g * hx_send[n, 0] + drop_right
        update_h((top_x, top_y))
        for z in range(cz):
            y_ = face_y[z : z + 1]
            if z == 0:
                y_ = y_ - g[0:1] * corner_b[n]
            h[1, z, at_x, :] = h[1, z, at_x, :] + 0.5 * face_z[z : z + 1]
            h[2, z, at_x, :] = h[2, z, at_x, :] - 0.5 * y_

        if n + 1 < STEPS:
            pack_h(n + 1)
            update_ez()
            if n + 2 < STEPS:
                send_pre(n + 2)
            send_h(n + 1)
            send_corners(n + 1)
            update_exy()
            send_e(n + 1)
        if n + 2 == STEPS:
            volt_out[...] = own_volts(src)

    wave_out[0, 0:1, :] = waves_a[-1][0:1]
    wave_out[0, 1:2, :] = waves_b[-1][0:1]

    for copy in info_copies:
        copy.wait_send()
    when(has_above, [line_copy], "wait_send")
    when(has_below, [gain_z], "wait_send")
    when(has_left, [gain_x], "wait_send")
    for n in range(STEPS):
        slab, up, down = y_copies(n)
        for copy in slab:
            copy.wait_send()
        when(has_above, up, "wait_send")
        when(has_below, down, "wait_send")
        if n:
            for copy in pre_copies(n):
                copy.wait_send()
        when(has_right, [up_x(n)], "wait_send")
        when(has_left, [down_x(n)], "wait_send")
        when(has_below & has_right, [corner_down(n)], "wait_send")
        when(has_above & has_left, [corner_up(n)], "wait_send")


def local(*args):
    e_field, inverse = args[0], args[7]
    nj = lax.axis_size("fxy")
    _, cz, cx, ny = e_field.shape
    _, block, nodes = inverse.shape
    ports, lines = args[4].shape[1], args[8].shape[1]
    args = [*args[:12], *(a.transpose(1, 0, 2) for a in args[12:])]
    depth = args[12].shape[0]
    vmem = pl.BlockSpec(memory_space=pltpu.VMEM)
    hbm = pl.BlockSpec(memory_space=pltpu.HBM)
    small = [a for i, a in enumerate(args) if i not in (0, 1, 2, 3, 7)]
    rows = -(-nj // 16) * 16
    np_ = nj * ports
    nt = np_ + 2 * lines
    line_rows = -(-(3 + 2 * depth) // 8) * 8
    dma = pltpu.SemaphoreType.DMA
    v = pltpu.VMEM
    e, h, volt, wave = pl.pallas_call(
        kernel,
        out_shape=(
            v(e_field.shape, F32),
            v(e_field.shape, F32),
            v((1, block), F32),
            v((1, 2, lines), F32),
        ),
        in_specs=[hbm] * len(args),
        out_specs=(vmem,) * 4,
        scratch_shapes=[
            *[v(a.shape, a.dtype) for a in small],
            v((cz, cx, ny), F32),
            v((cz, cx, ny), F32),
            v((cx, ny), F32),
            v((cz, ny), F32),
            v((cz, ny), F32),
            v((block, nodes), F32),
            v((2 * block, nodes), BF16),
            v((nodes, nt), BF16),
            v((2 * block, nt), BF16),
            v((nt, block), BF16),
            v((np_, np_), F32),
            v((2 * np_ + 2 * lines, block), BF16),
            v((nt, 2 * nt), BF16),
            v((cz * cx, LANES), F32),
            v((ny, LANES), BF16),
            v((cz, LANES), F32),
            v((ny, LANES), BF16),
            v((rows, nt), F32),
            v((block, nt), BF16),
            v((8, LANES), F32),
            v((8, LANES), F32),
            v((nj, 8, LANES), F32),
            v((line_rows, lines), F32),
            v((line_rows, lines), F32),
            v((STEPS, 1, np_), F32),
            v((STEPS, nj, 1, np_), F32),
            v((STEPS, 1, nt), F32),
            v((STEPS, nj, 1, nt), F32),
            v((STEPS, nj, 1, lines), F32),
            v((STEPS, nj, 1, lines), F32),
            v((STEPS, 2, cx, ny), F32),
            v((STEPS, 2, cx, ny), F32),
            v((STEPS, 2, cz, ny), F32),
            v((STEPS, 2, cz, ny), F32),
            v((STEPS, 2, cz, ny), F32),
            v((STEPS, 2, cz, ny), F32),
            v((STEPS, 2, 1, ny), F32),
            v((STEPS, 1, ny), F32),
            v((STEPS, 1, ny), F32),
            v((block, LANES), F32),
            dma((5 + len(small),)),
            dma((7, STEPS)),
            dma((7, STEPS)),
            dma((nj - 1,)),
            dma((nj - 1,)),
            dma((STEPS, nj - 1)),
            dma((STEPS, nj - 1)),
            dma((STEPS, nj - 1)),
            dma((STEPS, nj - 1)),
            dma((STEPS, nj)),
            dma((STEPS, nj)),
            dma((STEPS, nj)),
            dma((STEPS, nj)),
        ],
        compiler_params=pltpu.CompilerParams(
            collective_id=0, has_side_effects=True, vmem_limit_bytes=61 * 1024 * 1024
        ),
    )(*args)
    outs = [pltpu.with_memory_space_constraint(x, pltpu.VMEM) for x in (e, h, volt, wave)]
    return pl.pallas_call(
        store,
        out_shape=[jax.ShapeDtypeStruct(x.shape, F32) for x in outs],
        in_specs=[vmem] * 4,
        out_specs=[hbm] * 4,
        scratch_shapes=[dma((4,))],
    )(*outs)


def store(e, h, volt, wave, e_out, h_out, volt_out, wave_out, sem):
    pairs = ((e, e_out), (h, h_out), (volt, volt_out), (wave, wave_out))
    copies = [pltpu.make_async_copy(a, b, sem.at[k]) for k, (a, b) in enumerate(pairs)]
    for copy in copies:
        copy.start()
    for copy in copies:
        copy.wait()


def solution(mesh):
    placed = (
        P(None, "fz", "fxy", None),
        P(None, "fz", "fxy", None),
        P("fz", "fxy", None),
        P("fz", "fxy", None),
        P("fz", "fxy"),
        P("fz", "fxy"),
        P("fz", "fxy"),
        P("fz", "fxy", None),
        P("fz", None),
        P("fz", None),
        P("fz", None),
        P("fz", None),
        P("fz", None, None),
        P("fz", None, None),
    )
    return jax.shard_map(
        local,
        mesh=mesh,
        in_specs=placed,
        out_specs=(
            P(None, "fz", "fxy", None),
            P(None, "fz", "fxy", None),
            P("fz", "fxy"),
            P("fz", None, None),
        ),
        check_vma=False,
    )
```

```python
import jax
import jax.numpy as jnp
from jax import lax
from jax.experimental import pallas as pl
from jax.experimental.pallas import tpu as pltpu
from jax.sharding import PartitionSpec as P

STEPS = 4
LANES = 128
F32 = jnp.float32
BF16 = jnp.bfloat16
I32 = jnp.int32
MESH = pl.DeviceIdType.MESH
ROWS = (((1,), (0,)), ((), ()))
COLS = (((1,), (1,)), ((), ()))


def iota(shape, dim):
    return lax.broadcasted_iota(I32, shape, dim)


def parts3(x):
    a = x.astype(BF16).astype(F32)
    r = x - a
    b = r.astype(BF16).astype(F32)
    return a, b, r - b


def dot(x, y, dims=ROWS):
    return lax.dot_general(x, y, dims, preferred_element_type=F32)


def dot3(x, onehot, dims):
    rows = x.shape[0]
    parts = list(parts3(x))
    pad = -3 * rows % 16
    if pad:
        parts.append(jnp.zeros((pad, x.shape[1]), F32))
    y = dot(jnp.concatenate(parts, 0).astype(BF16), onehot, dims)
    return y[:rows] + y[rows : 2 * rows] + y[2 * rows : 3 * rows]


def fold3(x):
    a, b, c = parts3(jnp.broadcast_to(x, (16, x.shape[1])))
    r = iota(a.shape, 0)
    x = jnp.where(r == 0, a, jnp.where(r == 1, b, jnp.where(r == 2, c, 0.0)))
    return x.astype(BF16)


def sum3(y):
    return y[0:1] + y[1:2] + y[2:3]


def column(row):
    return jnp.concatenate(
        [
            jnp.broadcast_to(row[:, t : t + LANES], (LANES, LANES)).T
            for t in range(0, row.shape[1], LANES)
        ],
        0,
    )


def kernel(
    e_in, h_in, decay_in, gain_in, port_cell_in, port_node_in, port_cond_in, inv_in,
    line_near_in, line_far_in, line_delay_in, line_imped_in, hist_near_in, hist_far_in,
    e, h, volt_out, wave_out,
    port_cell, port_node, port_cond, line_near, line_far, line_delay, line_imped,
    hist_near, hist_far,
    decay, gain, gain_top, gain_send, gain_right, inv, inv2, pick, picked, own_pick,
    same, left, mat, cell_row, cell_y, row_right, y_right, node_hi, node_lo, pads,
    info_send, info, line_send, line_info, pre_send, pre, y_send, y, below, above,
    hz, ez_up, hx_send, hx, ex_send, ex, corner_send, corner_a, corner_b, acc,
    load_sem, face_ss, face_rs, info_ss, info_rs, pre_ss, pre_rs, y_ss, y_rs,
    up_ss, up_rs, down_ss, down_rs,
):
    s, j = lax.axis_index("fz"), lax.axis_index("fxy")
    ns, nj = lax.axis_size("fz"), lax.axis_size("fxy")
    above_id, below_id = lax.rem(s + 1, ns), lax.rem(s + ns - 1, ns)
    right_id, left_id = lax.rem(j + 1, nj), lax.rem(j + nj - 1, nj)
    has_above, has_below = s < ns - 1, s > 0
    has_right, has_left = j < nj - 1, j > 0
    _, cz, cx, ny = e_in.shape
    cells = cz * cx
    block, nodes = inv_in.shape[1:]
    ports = port_cell_in.shape[1]
    lines = line_near_in.shape[1]
    depth = hist_near_in.shape[0]
    pack = LANES // ports
    tiles = nj // pack
    np_ = nj * ports
    nt = np_ + 2 * lines

    loads = [
        pltpu.make_async_copy(e_in, e, load_sem.at[0]),
        pltpu.make_async_copy(gain_in, gain, load_sem.at[1]),
        pltpu.make_async_copy(h_in, h, load_sem.at[2]),
        pltpu.make_async_copy(decay_in, decay, load_sem.at[3]),
        pltpu.make_async_copy(inv_in.at[0], inv, load_sem.at[4]),
    ]
    small = (
        (port_cell_in, port_cell), (port_node_in, port_node), (port_cond_in, port_cond),
        (line_near_in, line_near), (line_far_in, line_far), (line_delay_in, line_delay),
        (line_imped_in, line_imped), (hist_near_in, hist_near), (hist_far_in, hist_far),
    )
    small = [
        pltpu.make_async_copy(src, dst, load_sem.at[5 + k])
        for k, (src, dst) in enumerate(small)
    ]
    for copy in small + loads[:4]:
        copy.start()

    below[...] = jnp.zeros(below.shape, F32)
    above[...] = jnp.zeros(above.shape, F32)
    corner_a[...] = jnp.zeros(corner_a.shape, F32)
    corner_b[...] = jnp.zeros(corner_b.shape, F32)
    line_info[...] = (iota(line_info.shape, 0) == 2).astype(F32)

    barrier = pltpu.get_barrier_semaphore()
    for other in (above_id, below_id):
        pl.semaphore_signal(barrier, inc=1, device_id={"fz": other}, device_id_type=MESH)
    for d in range(1, nj):
        pl.semaphore_signal(
            barrier, inc=1, device_id={"fxy": lax.rem(j + d, nj)}, device_id_type=MESH
        )

    for missing, refs in (
        (jnp.logical_not(has_below), (hz,)),
        (jnp.logical_not(has_above), (ez_up, gain_top)),
        (jnp.logical_not(has_left), (hx,)),
        (jnp.logical_not(has_right), (ex, gain_right)),
    ):

        @pl.when(missing)
        def _(refs=refs):
            for ref in refs:
                ref[...] = jnp.zeros(ref.shape, F32)

    def remote(src, dst, ss, rs, **where):
        return pltpu.make_async_remote_copy(
            src_ref=src, dst_ref=dst, send_sem=ss, recv_sem=rs,
            device_id=where, device_id_type=MESH,
        )

    def face(kind, n, src, dst, **where):
        return remote(src, dst, face_ss.at[kind, n], face_rs.at[kind, n], **where)

    def when(cond, copies, act):
        @pl.when(cond)
        def _():
            for copy in copies:
                getattr(copy, act)()

    def up_z(n):
        return face(0, n, h.at[0:2, cz - 1], hz.at[n], fz=above_id)

    def up_x(n):
        return face(1, n, hx_send.at[n], hx.at[n], fxy=right_id)

    def down_z(n):
        return face(2, n, e.at[0:2, 0], ez_up.at[n], fz=below_id)

    def down_x(n):
        return face(3, n, ex_send.at[n], ex.at[n], fxy=left_id)

    def corner_down(n):
        return face(4, n, corner_send.at[n, 0], corner_a.at[n], fz=below_id, fxy=right_id)

    def corner_up(n):
        return face(5, n, corner_send.at[n, 1], corner_b.at[n], fz=above_id, fxy=left_id)

    line_copy = face(6, 0, line_send, line_info, fz=above_id)
    gain_z = face(6, 1, gain.at[0], gain_top, fz=below_id)
    gain_x = face(6, 2, gain_send, gain_right, fxy=left_id)

    def spread(src, dst, ss, rs):
        return [
            remote(src, dst, ss.at[d - 1], rs.at[d - 1], fxy=lax.rem(j + d, nj))
            for d in range(1, nj)
        ]

    def spread_z(src, dst, ss, rs, to):
        return [
            remote(src, dst, ss.at[d], rs.at[d], fz=to, fxy=lax.rem(j + d, nj))
            for d in (*range(1, nj), 0)
        ]

    info_copies = spread(info_send, info.at[j], info_ss, info_rs)

    def pre_copies(n):
        return spread(pre_send.at[n], pre.at[n, j], pre_ss.at[n], pre_rs.at[n])

    def y_copies(n):
        return (
            spread(y_send.at[n], y.at[n, j], y_ss.at[n], y_rs.at[n]),
            spread_z(
                y_send.at[n, :, np_ : np_ + lines], below.at[n, j],
                up_ss.at[n], up_rs.at[n], above_id,
            ),
            spread_z(
                y_send.at[n, :, np_ + lines : nt], above.at[n, j],
                down_ss.at[n], down_rs.at[n], below_id,
            ),
        )

    def send_y(n, value):
        y_send[n] = value
        y[n, j] = value
        slab, up, down = y_copies(n)
        when(has_above, up, "start")
        when(has_below, down, "start")
        for copy in slab:
            copy.start()

    def pack_h(n):
        for c in range(2):
            for z in range(cz):
                hx_send[n, c, z : z + 1, :] = h[1 + c, z, cx - 1 : cx, :]
        corner_send[n, 0] = h[2, 0, cx - 1 : cx, :]
        corner_send[n, 1] = h[0, cz - 1, 0:1, :]

    def send_h(n):
        when(has_above, [up_z(n)], "start")
        when(has_right, [up_x(n)], "start")

    def send_corners(n):
        when(has_below & has_right, [corner_down(n)], "start")
        when(has_above & has_left, [corner_up(n)], "start")

    def send_e(n):
        for c in range(2):
            for z in range(cz):
                ex_send[n, c, z : z + 1, :] = e[1 + c, z, 0:1, :]
        when(has_below, [down_z(n)], "start")
        when(has_left, [down_x(n)], "start")

    lane = iota((cx, ny), 1)
    sub = iota((cx, ny), 0)

    def by(f):
        return f - jnp.where(lane == 0, 0.0, pltpu.roll(f, 1, 1))

    def bx(f):
        return f - jnp.where(sub == 0, 0.0, pltpu.roll(f, 1, 0))


    def update_ez():
        for z in range(cz):
            e[2, z] = decay[z] * e[2, z] + gain[z] * (bx(h[1, z]) - by(h[0, z]))

    def update_exy():
        for z in range(cz):
            dx, dy, hz_ = h[0, z], h[1, z], h[2, z]
            if z:
                dx, dy = dx - h[0, z - 1], dy - h[1, z - 1]
            e[0, z] = decay[z] * e[0, z] + gain[z] * (by(hz_) - dy)
            e[1, z] = decay[z] * e[1, z] + gain[z] * (dx - bx(hz_))

    def update_h(top):
        def plane(z, ux, uy):
            ex_, ey_, ez_ = (e[c, z] for c in range(3))

            def dy(f):
                return jnp.where(lane == ny - 1, 0.0, pltpu.roll(f, ny - 1, 1)) - f

            def dx(f):
                return jnp.where(sub == cx - 1, 0.0, pltpu.roll(f, cx - 1, 0)) - f

            h[0, z] = h[0, z] - 0.5 * (dy(ez_) - (uy - ey_))
            h[1, z] = h[1, z] - 0.5 * ((ux - ex_) - dx(ez_))
            h[2, z] = h[2, z] - 0.5 * (dx(ey_) - dy(ex_))

        @pl.loop(0, cz - 1, unroll=True)
        def _(z):
            plane(z, e[0, z + 1], e[1, z + 1])

        plane(cz - 1, *top)

    for copy in small:
        copy.wait()

    pads[...] = jnp.zeros(pads.shape, F32)
    pads[0:1, 0:ports] = (port_cell[...] + 1).astype(F32)
    pads[1:2, 0:ports] = (port_node[...] + 1).astype(F32)
    pads[2:3, 0:ports] = port_cond[...]
    rows = pltpu.roll(pads[...], ports * lax.rem(j, pack), 1)
    info_send[...] = rows
    cell = rows[0:1].astype(I32) - 1
    valid = cell >= 0
    cell_row[...] = (
        iota((cells, LANES), 0) == jnp.where(valid, cell // ny, -1)
    ).astype(F32)
    cell_y[...] = (
        (iota((ny, LANES), 0) == jnp.where(valid, cell % ny, -1)).astype(F32).astype(BF16)
    )
    line_send[...] = jnp.zeros(line_send.shape, F32)
    line_send[0:1, :] = (line_far[...] + 1).astype(F32)
    line_send[1:2, :] = line_delay[...].astype(F32)
    line_send[2:3, :] = line_imped[...]
    for k in range(depth):
        line_send[3 + k : 4 + k, :] = hist_near[k]
        line_send[3 + depth + k : 4 + depth + k, :] = hist_far[k]

    def gather_cells(f):
        value = dot3(f.reshape(cells, ny), cell_y[...], ROWS)
        return jnp.sum(value * cell_row[...], axis=0, keepdims=True)

    loads[0].wait()
    loads[4].start()
    info_send[4:5, :] = gather_cells(e[2])
    loads[1].wait()
    info_send[3:4, :] = gather_cells(gain[...])
    for z in range(cz):
        gain_send[z : z + 1, :] = gain[z, 0:1, :]
    info[j] = info_send[...]

    pl.semaphore_wait(barrier, nj + 1)
    for copy in info_copies:
        copy.start()
    when(has_above, [line_copy], "start")
    when(has_below, [gain_z], "start")
    loads[2].wait()
    pack_h(0)
    send_h(0)
    when(has_left, [gain_x], "start")
    loads[3].wait()
    update_ez()
    update_exy()
    send_e(0)
    loads[4].wait()

    chunk = 32

    @pl.loop(0, block // chunk, unroll=4)
    def _(r):
        at = pl.ds(pl.multiple_of(r * chunk, chunk), chunk)
        x = inv[at, :]
        high = x.astype(BF16)
        inv2[at, :] = high
        inv2[pl.ds(pl.multiple_of(block + r * chunk, chunk), chunk), :] = (
            x - high.astype(F32)
        ).astype(BF16)

    wide = 2 * LANES

    def take_columns(first, last, index):
        @pl.loop(0, nodes // LANES, unroll=4)
        def _(r):
            at = pl.ds(pl.multiple_of(r * LANES, LANES), LANES)
            hit = iota((LANES, last - first), 0) + r * LANES == index
            pick[at, first:last] = hit.astype(F32).astype(BF16)

        for c in range(first, last, wide):
            at = slice(c, min(c + wide, last))
            for half in range(2):
                rows = slice(half * block, (half + 1) * block)
                picked[rows, at] = dot(inv2[rows, :], pick[:, at]).astype(BF16)

    when(has_above, [gain_z], "wait_recv")
    when(has_below, [line_copy], "wait_recv")
    send_corners(0)
    near_far = jnp.concatenate([line_near[...], line_info[0:1, :].astype(I32) - 1], 1)
    for copy in info_copies:
        copy.wait_recv()

    everyone = jnp.concatenate(
        [sum(info[t * pack + k] for k in range(pack)) for t in range(tiles)], 1
    )
    cell_all = everyone[0:1] - 1.0
    cond_all, gain_all = everyone[2:3], everyone[3:4]
    index = jnp.concatenate([everyone[1:2].astype(I32) - 1, near_far], 1)
    high = jnp.where(index >= 0, index // block, -1)
    low = jnp.where(index >= 0, index % block, -1)
    node_hi[...] = (iota(node_hi.shape, 0) == high).astype(F32)
    node_lo[...] = (iota(node_lo.shape, 0) == low).astype(F32).astype(BF16)

    delay = jnp.concatenate([line_delay[...].astype(F32), line_info[1:2, :]], 0)
    scale = -2.0 / jnp.concatenate([line_imped[...], line_info[2:3, :]], 0)
    past_a = [
        jnp.concatenate([hist_near[k], line_info[3 + k : 4 + k, :]], 0)
        for k in range(depth)
    ]
    past_b = [
        jnp.concatenate([hist_far[k], line_info[3 + depth + k : 4 + depth + k, :]], 0)
        for k in range(depth)
    ]
    waves_a, waves_b = [], []

    def incoming(n, waves, past):
        total = jnp.zeros((2, lines), F32)
        for k in range(1, depth + 1):
            value = waves[n - k] if n >= k else past[k - n - 1]
            total = jnp.where(delay == k, value, total)
        return total

    def sources(n, ez):
        in_a, in_b = incoming(n, waves_b, past_b), incoming(n, waves_a, past_a)
        return in_a, in_b, jnp.concatenate([cond_all * ez, -in_a[0:1], -in_b[1:2]], 1)

    def own_volts(src):
        totals = dot3(node_hi[...] * src, node_lo[...], COLS)[0:nj]

        @pl.loop(0, block // chunk, unroll=4)
        def _(r):
            at = pl.ds(pl.multiple_of(r * chunk, chunk), chunk)
            value = jnp.zeros((chunk, LANES), F32)
            for k in range(nodes // LANES):
                q, w = divmod(k * LANES, block)
                value = value + inv[at, k * LANES : (k + 1) * LANES] * totals[
                    q : q + 1, w : w + LANES
                ]
            acc[at, :] = value

        terms = jnp.concatenate(parts3(acc[...]), 1).astype(BF16)
        return dot(jnp.ones((16, 3 * LANES), BF16), terms, COLS)[0:1]

    key = cell_all + ((iota((1, np_), 1) // ports) * (cells * ny)).astype(F32)
    key_col = column(key)
    for t in range(0, np_, LANES):
        at = slice(t, t + LANES)
        same[:, at] = (key_col == key[:, at]).astype(F32) * cond_all[:, at]

    ez = everyone[4:5]
    in_a, in_b, src = sources(0, ez)
    v0 = sum3(dot(fold3(own_volts(src)), node_lo[...]))
    v0 = jnp.where(high == j, v0, 0.0)
    drive = lax.dot_general(
        jnp.broadcast_to(v0[:, 0:np_], (8, np_)), same[...], COLS,
        precision=lax.Precision.HIGHEST, preferred_element_type=F32,
    )[0:1]
    send_y(0, jnp.concatenate([gain_all * drive, v0[:, np_:]], 1))

    neighbour = info[right_id]
    cell_r = neighbour[0:1].astype(I32) - 1
    gain_r = neighbour[3:4]
    valid_r = (cell_r >= 0) & (lax.rem(cell_r // ny, cx) == 0) & has_right
    row_right[...] = (
        iota((cz, LANES), 0) == jnp.where(valid_r, cell_r // (cx * ny), -1)
    ).astype(F32)
    y_right[...] = (
        (iota((ny, LANES), 0) == jnp.where(valid_r, cell_r % ny, -1))
        .astype(F32)
        .astype(BF16)
    )

    def send_pre(n):
        value = gather_cells(e[2])
        side = dot3(hx_send[n - 1, 0], y_right[...], ROWS) * row_right[...]
        side = -gain_r * jnp.sum(side, axis=0, keepdims=True)
        for t in range(tiles):
            at = slice(t * LANES, (t + 1) * LANES)
            both = jnp.where(j // pack == t, value, 0.0)
            both = both + jnp.where(right_id // pack == t, side, 0.0)
            pre_send[n, :, at] = both
        pre[n, j] = pre_send[n]
        for copy in pre_copies(n):
            copy.start()

    send_pre(1)

    cond_col = column(cond_all)
    gain_col = column(gain_all)
    load, first = [], []
    for t in range(0, np_, LANES):
        hit = key_col == key[:, t : t + LANES]
        load.append(jnp.sum(jnp.where(hit, cond_col, 0.0), axis=0, keepdims=True))
        earlier = hit & (iota(hit.shape, 0) < iota(hit.shape, 1) + t)
        first.append(jnp.max(earlier.astype(F32), axis=0, keepdims=True))
    load = gain_all * jnp.concatenate(load, 1)
    first = 1.0 - jnp.concatenate(first, 1)

    take_columns(0, nt, index)
    index_col = column(index.astype(F32))
    for w in range(0, block, LANES):
        node = (iota((nt, LANES), 1) + (w + j * block)).astype(F32)
        own_pick[:, w : w + LANES] = (index_col == node).astype(F32).astype(BF16)
    mixed = dot3(same[...], own_pick[0:np_, :], ROWS)
    for w in range(0, block, LANES):
        at = slice(w, w + LANES)
        value = mixed[:, at] * gain_col
        high_ = value.astype(BF16)
        left[0:np_, at] = high_
        left[np_ : 2 * np_, at] = (value - high_.astype(F32)).astype(BF16)
    left[2 * np_ :, :] = own_pick[np_:, :]
    upper = dot(left[...], picked[0:block, :])
    lower = dot(left[0:np_, :], picked[block:, :])
    value = upper[0:np_] + (upper[np_ : 2 * np_] + lower)
    high_ = value.astype(BF16)
    mat[0:np_, 0:nt] = high_
    mat[0:np_, nt:] = (value - high_.astype(F32)).astype(BF16)
    mat[np_:, 0:nt] = upper[2 * np_ :].astype(BF16)
    mat[np_:, nt:] = dot(left[2 * np_ :, :], picked[block:, :]).astype(BF16)

    def tile_of(x, device):
        out = x[:, 0:LANES]
        for t in range(1, tiles):
            out = jnp.where(device // pack == t, x[:, t * LANES : (t + 1) * LANES], out)
        return out

    when(has_right, [gain_x], "wait_recv")
    at_x = slice(cx - 1, cx)

    for n in range(STEPS):
        slab, up, down = y_copies(n)
        for copy in slab:
            copy.wait_recv()
        when(has_below, up, "wait_recv")
        when(has_above, down, "wait_recv")
        total, v_below, v_above = y[n, 0], below[n, 0], above[n, 0]
        for k in range(1, nj):
            total = total + y[n, k]
            v_below = v_below + below[n, k]
            v_above = v_above + above[n, k]
        v_near = jnp.concatenate([total[:, np_ : np_ + lines], v_below], 0)
        v_far = jnp.concatenate([v_above, total[:, np_ + lines :]], 0)
        waves_a.append(scale * v_near - in_a)
        waves_b.append(scale * v_far - in_b)
        change = total[:, 0:np_] - load * ez
        once = change * first
        drop = dot3(cell_row[...] * tile_of(once, j), cell_y[...], COLS)

        if n + 1 < STEPS:
            for copy in pre_copies(n + 1):
                copy.wait_recv()
            ez = change + pre[n + 1, 0]
            for k in range(1, nj):
                ez = ez + pre[n + 1, k]
            in_a, in_b, src = sources(n + 1, ez)
            x = fold3(src)
            send_y(n + 1, sum3(dot(jnp.concatenate([x, x], 1), mat[...], COLS)))
        when(has_below, [down_z(n)], "wait_send")
        when(has_above, [up_z(n)], "wait_send")
        when(has_left, [up_x(n)], "wait_recv")
        when(has_below, [up_z(n)], "wait_recv")
        when(has_above, [down_z(n)], "wait_recv")
        when(has_right, [down_x(n)], "wait_recv")
        when(has_above & has_left, [corner_down(n)], "wait_recv")
        when(has_below & has_right, [corner_up(n)], "wait_recv")
        for z in range(cz):
            g = gain[z, 0:1, :]
            e[1, z, 0:1, :] = e[1, z, 0:1, :] + g * hx[n, 1, z : z + 1, :]
            e[2, z, 0:1, :] = e[2, z, 0:1, :] - g * hx[n, 0, z : z + 1, :]
        e[0, 0] = e[0, 0] + gain[0] * hz[n, 1]
        e[1, 0] = e[1, 0] - gain[0] * hz[n, 0]
        e[2] = e[2] + drop.reshape(cz, cx, ny)
        top_x = ez_up[n, 0] + gain_top[...] * h[1, cz - 1]
        side = jnp.where(sub == 0, gain_top[0:1, :] * corner_a[n], 0.0)
        top_y = ez_up[n, 1] - gain_top[...] * h[0, cz - 1] + side
        drop_right = dot3(row_right[...] * tile_of(once, right_id), y_right[...], COLS)
        g = gain_right[...]
        face_y = ex[n, 0] + g * hx_send[n, 1]
        face_z = ex[n, 1] - g * hx_send[n, 0] + drop_right
        update_h((top_x, top_y))
        for z in range(cz):
            y_ = face_y[z : z + 1]
            if z == 0:
                y_ = y_ - g[0:1] * corner_b[n]
            h[1, z, at_x, :] = h[1, z, at_x, :] + 0.5 * face_z[z : z + 1]
            h[2, z, at_x, :] = h[2, z, at_x, :] - 0.5 * y_

        if n + 1 < STEPS:
            pack_h(n + 1)
            update_ez()
            if n + 2 < STEPS:
                send_pre(n + 2)
            send_h(n + 1)
            send_corners(n + 1)
            update_exy()
            send_e(n + 1)
        if n + 2 == STEPS:
            volt_out[...] = own_volts(src)

    wave_out[0, 0:1, :] = waves_a[-1][0:1]
    wave_out[0, 1:2, :] = waves_b[-1][0:1]

    for copy in info_copies:
        copy.wait_send()
    when(has_above, [line_copy], "wait_send")
    when(has_below, [gain_z], "wait_send")
    when(has_left, [gain_x], "wait_send")
    for n in range(STEPS):
        slab, up, down = y_copies(n)
        for copy in slab:
            copy.wait_send()
        when(has_above, up, "wait_send")
        when(has_below, down, "wait_send")
        if n:
            for copy in pre_copies(n):
                copy.wait_send()
        when(has_right, [up_x(n)], "wait_send")
        when(has_left, [down_x(n)], "wait_send")
        when(has_below & has_right, [corner_down(n)], "wait_send")
        when(has_above & has_left, [corner_up(n)], "wait_send")


def local(*args):
    e_field, inverse = args[0], args[7]
    nj = lax.axis_size("fxy")
    _, cz, cx, ny = e_field.shape
    _, block, nodes = inverse.shape
    ports, lines = args[4].shape[1], args[8].shape[1]
    args = [*args[:12], *(a.transpose(1, 0, 2) for a in args[12:])]
    depth = args[12].shape[0]
    vmem = pl.BlockSpec(memory_space=pltpu.VMEM)
    hbm = pl.BlockSpec(memory_space=pltpu.HBM)
    small = [a for i, a in enumerate(args) if i not in (0, 1, 2, 3, 7)]
    rows = -(-nj // 16) * 16
    np_ = nj * ports
    nt = np_ + 2 * lines
    line_rows = -(-(3 + 2 * depth) // 8) * 8
    dma = pltpu.SemaphoreType.DMA
    v = pltpu.VMEM
    e, h, volt, wave = pl.pallas_call(
        kernel,
        out_shape=(
            v(e_field.shape, F32),
            v(e_field.shape, F32),
            v((1, block), F32),
            v((1, 2, lines), F32),
        ),
        in_specs=[hbm] * len(args),
        out_specs=(vmem,) * 4,
        scratch_shapes=[
            *[v(a.shape, a.dtype) for a in small],
            v((cz, cx, ny), F32),
            v((cz, cx, ny), F32),
            v((cx, ny), F32),
            v((cz, ny), F32),
            v((cz, ny), F32),
            v((block, nodes), F32),
            v((2 * block, nodes), BF16),
            v((nodes, nt), BF16),
            v((2 * block, nt), BF16),
            v((nt, block), BF16),
            v((np_, np_), F32),
            v((2 * np_ + 2 * lines, block), BF16),
            v((nt, 2 * nt), BF16),
            v((cz * cx, LANES), F32),
            v((ny, LANES), BF16),
            v((cz, LANES), F32),
            v((ny, LANES), BF16),
            v((rows, nt), F32),
            v((block, nt), BF16),
            v((8, LANES), F32),
            v((8, LANES), F32),
            v((nj, 8, LANES), F32),
            v((line_rows, lines), F32),
            v((line_rows, lines), F32),
            v((STEPS, 1, np_), F32),
            v((STEPS, nj, 1, np_), F32),
            v((STEPS, 1, nt), F32),
            v((STEPS, nj, 1, nt), F32),
            v((STEPS, nj, 1, lines), F32),
            v((STEPS, nj, 1, lines), F32),
            v((STEPS, 2, cx, ny), F32),
            v((STEPS, 2, cx, ny), F32),
            v((STEPS, 2, cz, ny), F32),
            v((STEPS, 2, cz, ny), F32),
            v((STEPS, 2, cz, ny), F32),
            v((STEPS, 2, cz, ny), F32),
            v((STEPS, 2, 1, ny), F32),
            v((STEPS, 1, ny), F32),
            v((STEPS, 1, ny), F32),
            v((block, LANES), F32),
            dma((5 + len(small),)),
            dma((7, STEPS)),
            dma((7, STEPS)),
            dma((nj - 1,)),
            dma((nj - 1,)),
            dma((STEPS, nj - 1)),
            dma((STEPS, nj - 1)),
            dma((STEPS, nj - 1)),
            dma((STEPS, nj - 1)),
            dma((STEPS, nj)),
            dma((STEPS, nj)),
            dma((STEPS, nj)),
            dma((STEPS, nj)),
        ],
        compiler_params=pltpu.CompilerParams(
            collective_id=0, has_side_effects=True, vmem_limit_bytes=61 * 1024 * 1024
        ),
    )(*args)
    outs = [pltpu.with_memory_space_constraint(x, pltpu.VMEM) for x in (e, h, volt, wave)]
    return pl.pallas_call(
        store,
        out_shape=[jax.ShapeDtypeStruct(x.shape, F32) for x in outs],
        in_specs=[vmem] * 4,
        out_specs=[hbm] * 4,
        scratch_shapes=[dma((4,))],
    )(*outs)


def store(e, h, volt, wave, e_out, h_out, volt_out, wave_out, sem):
    pairs = ((e, e_out), (h, h_out), (volt, volt_out), (wave, wave_out))
    copies = [pltpu.make_async_copy(a, b, sem.at[k]) for k, (a, b) in enumerate(pairs)]
    for copy in copies:
        copy.start()
    for copy in copies:
        copy.wait()


def solution(mesh):
    placed = (
        P(None, "fz", "fxy", None),
        P(None, "fz", "fxy", None),
        P("fz", "fxy", None),
        P("fz", "fxy", None),
        P("fz", "fxy"),
        P("fz", "fxy"),
        P("fz", "fxy"),
        P("fz", "fxy", None),
        P("fz", None),
        P("fz", None),
        P("fz", None),
        P("fz", None),
        P("fz", None, None),
        P("fz", None, None),
    )
    return jax.shard_map(
        local,
        mesh=mesh,
        in_specs=placed,
        out_specs=(
            P(None, "fz", "fxy", None),
            P(None, "fz", "fxy", None),
            P("fz", "fxy"),
            P("fz", None, None),
        ),
        check_vma=False,
    )
```
